512 devices in a mesh: ma: 64 (over z, x, core), ell: 8 (over y).
Axes of the slice: x: 4, y: 8, z: 8, core: 2. Of those that a mesh axis runs over, the one named last changes fastest.
Arguments:
- legendre: bfloat16 [3, 2048, 32, 4096], P(None, 'ma', None, 'ell'), may hold values from -6 to 6
- harmonics: bfloat16 [2048, 3, 2, 4, 4096], P('ma', None, None, None, 'ell'), may hold values from -0.0014648438 to 0.0014648438
- slot_orders: int32 [2048], replicated, may hold values from 0 to 2047, each once
- cycle_index: int32 [32], replicated, may hold values from 2048 to 4095
Outputs:
- maps: float32 [64, 3, 4, 8192], P('ma', None, None, 'ell')
The draws below stay inside these ranges and needn't reach their ends.
Inputs may be any that keep to these rules, and one draw needn't show every extreme that they name: `slot_orders`: every number from 0 to 2047 appears once.
All inputs are finite; a program needn't handle non-finite values.
Results may differ from the reference program's by a relative error of at most 0.0003.
Values sent between devices are 32-bit elements; how exact they have to be, the bound alone decides.
No kernel may reach another device: no remote copies, remote signals or barrier semaphores. Data moves between devices by JAX's collectives and lax.ppermute only.
A program may use at most 64 MiB of HBM per device.

```python
import math
import jax
import jax.numpy as jnp
from jax import lax

L = 4096
COMPS = 4
SLOTS = 2048
NPIX = 8192
RPAIRS = 32


def plant(values, stream_key, smallest, high):
    extent = values.shape
    place = [jax.random.randint(jax.random.fold_in(stream_key, axis), (), 0, extent[axis]) for axis in range(len(extent))]
    values = values.at[tuple(place)].set(smallest)
    longest = extent.index(max(extent))
    place[longest] = (place[longest] + 1) % extent[longest]
    return values.at[tuple(place)].set(high)


def steps_of(rng, dims, split, low, largest):
    gain, own = 1.0, jax.random.fold_in(rng, 6)
    for dim, shards_of in split:
        draws = jnp.exp(jax.random.uniform(jax.random.fold_in(own, dim), (shards_of,), jnp.float32, low / len(split), largest / len(split)))
        gain = gain * jnp.repeat(draws, dims[dim] // shards_of).reshape([-1 if axis == dim else 1 for axis in range(len(dims))])
    return gain


def noise(stream_key, extent, spread, bound, shards=(), held_as=jnp.bfloat16):
    values = jax.random.normal(stream_key, extent, jnp.float32) * spread
    if len(shards) > 0:
        values = steps_of(stream_key, extent, shards, -0.22, 0.18) * values
    return jnp.clip(values, min=-bound, max=bound).astype(held_as)


def setup_inputs(seed: int = 0) -> dict:
    splits = jax.random.split(jax.random.key(seed), 5)
    legendre = noise(splits[0], (3, SLOTS, RPAIRS, L), 1.0, 6.0, ((1, 64), (3, 8)))
    harmonics = noise(splits[1], (SLOTS, 3, 2, COMPS, L), (L * L) ** -0.5, 0.0014648438, ((0, 64), (4, 8)))
    slot_orders = jax.random.permutation(splits[2], SLOTS).astype(jnp.int32)
    cycle_index = plant(jax.random.randint(splits[3], (RPAIRS,), L // 2, L), jax.random.fold_in(splits[3], 1), L // 2, L - 1).astype(jnp.int32)
    return {"legendre": legendre, "harmonics": harmonics, "slot_orders": slot_orders, "cycle_index": cycle_index}


def column_weights(lower_order, first_column, columns_count, full_width):
    columns = first_column + jnp.arange(columns_count, dtype=jnp.int32)
    boundary = (full_width - 1 - lower_order)[:, None]
    lower_part = (columns[None, :] < boundary).astype(jnp.float32)
    upper_part = ((columns[None, :] >= boundary) & (columns[None, :] < full_width - 1)).astype(jnp.float32)
    lower_sign = (1 - 2 * (columns[None, :] % 2)).astype(jnp.float32)
    upper_sign = (1 - 2 * ((columns[None, :] + 1 + lower_order[:, None]) % 2)).astype(jnp.float32)
    return jnp.stack([lower_part, lower_part * lower_sign, upper_part, upper_part * upper_sign], axis=1)


def spin_fields(plain, plus, minus):
    hemisphere = jnp.array([1.0, -1.0], jnp.float32).reshape(1, 1, 1, 2, 1, 1, 1)
    minus = minus * hemisphere
    temp_real = plain[:, :, :, :, 0]
    temp_imag = plain[:, :, :, :, 1]
    eplus_real = plus[:, :, :, :, 0, 0]
    eplus_imag = plus[:, :, :, :, 0, 1]
    bplus_real = plus[:, :, :, :, 1, 0]
    bplus_imag = plus[:, :, :, :, 1, 1]
    eminus_real = minus[:, :, :, :, 0, 0]
    eminus_imag = minus[:, :, :, :, 0, 1]
    bminus_real = minus[:, :, :, :, 1, 0]
    bminus_imag = minus[:, :, :, :, 1, 1]
    stokes_q_real = -(eplus_real - bminus_imag)
    stokes_q_imag = -(eplus_imag + bminus_real)
    stokes_u_real = -(bplus_real + eminus_imag)
    stokes_u_imag = -(bplus_imag - eminus_real)
    return jnp.stack([jnp.stack([temp_real, temp_imag]), jnp.stack([stokes_q_real, stokes_q_imag]), jnp.stack([stokes_u_real, stokes_u_imag])])


def reference(legendre, harmonics, slot_orders, cycle_index):
    highest = lax.Precision.HIGHEST
    block = min(16, SLOTS)

    def one_block(index):
        start = index * block
        tables = lax.dynamic_slice_in_dim(legendre, start, block, 1).astype(jnp.float32)
        coeffs = lax.dynamic_slice_in_dim(harmonics, start, block, 0).astype(jnp.float32)
        lower_order = lax.dynamic_slice_in_dim(slot_orders, start, block, 0)
        weights = column_weights(lower_order, 0, L, L)
        packed = coeffs[:, None] * weights[:, :, None, None, None, :]
        plain = jnp.einsum('srj,sqpcj->srqpc', tables[0], packed[:, :, 0], precision=highest)
        plus = jnp.einsum('srj,sqkpcj->srqkpc', tables[1], packed[:, :, 1:3], precision=highest)
        minus = jnp.einsum('srj,sqkpcj->srqkpc', tables[2], packed[:, :, 1:3], precision=highest)
        plain = plain.reshape(block, RPAIRS, 2, 2, 2, COMPS)
        plus = plus.reshape(block, RPAIRS, 2, 2, 2, 2, COMPS)
        minus = minus.reshape(block, RPAIRS, 2, 2, 2, 2, COMPS)
        return spin_fields(plain, plus, minus)

    blocks = lax.map(one_block, jnp.arange(SLOTS // block, dtype=jnp.int32))
    cycle_sums = blocks.transpose(6, 4, 1, 2, 7, 5, 0, 3).reshape(2 * RPAIRS, 3, 2, COMPS, 2, SLOTS)
    lower_all = slot_orders
    upper_all = L - 1 - lower_all
    coeff = jnp.zeros((2 * RPAIRS, 3, 2, COMPS, L), jnp.float32)
    coeff = coeff.at[..., lower_all].set(cycle_sums[..., 0, :]).at[..., upper_all].set(cycle_sums[..., 1, :])
    shift = jnp.concatenate([cycle_index, cycle_index]) % 2
    orders = jnp.arange(L, dtype=jnp.int32)
    phase = ((orders[None, :] * shift[:, None]) % (2 * NPIX)).astype(jnp.float32) * (math.pi / NPIX)
    factor = jnp.where(orders == 0, 1.0, 2.0).astype(jnp.float32)
    cosine = (jnp.cos(phase) * factor)[:, None, None, :]
    sine = (jnp.sin(phase) * factor)[:, None, None, :]
    real_part = coeff[:, :, 0]
    imag_part = coeff[:, :, 1]
    shifted_real = real_part * cosine - imag_part * sine
    shifted_imag = real_part * sine + imag_part * cosine
    spectrum = shifted_real + 1j * shifted_imag
    padded = jnp.pad(spectrum, ((0, 0), (0, 0), (0, 0), (0, NPIX - L)))
    maps = jnp.real(jnp.fft.ifft(padded, axis=-1)) * NPIX
    return maps.astype(jnp.float32)
```

```python
import math

import jax
import jax.numpy as jnp
from jax import lax
from jax.experimental import pallas as pl
from jax.experimental.pallas import tpu as pltpu
from jax.sharding import PartitionSpec as P

F32 = jnp.float32
BF16 = jnp.bfloat16
NT = (((1,), (1,)), ((), ()))


def legendre_kernel(orders_ref, leg_ref, harm_ref, out_ref, pack_ref, acc_ref):
    group = pl.program_id(0)
    groups = pl.num_programs(0)
    pairs = leg_ref.shape[2]
    width = leg_ref.shape[3]
    full = orders_ref[0]
    column = orders_ref[1] + lax.broadcasted_iota(jnp.int32, (1, width), 1)
    column_sign = (1 - 2 * (column % 2)).astype(F32)
    half = lax.broadcasted_iota(jnp.int32, (8, width), 0) < 4
    for slot in range(8):
        lower = orders_ref[2 + group * 8 + slot]
        boundary = full - 1 - lower
        lower_part = jnp.where(column < boundary, 1.0, 0.0).astype(F32)
        upper_part = jnp.where((column >= boundary) & (column < full - 1), 1.0, 0.0).astype(F32)
        upper_sign = column_sign * (2 * (lower % 2) - 1).astype(F32)
        temp = harm_ref[slot, 0].astype(F32)
        emode = harm_ref[slot, 1].astype(F32)
        bmode = harm_ref[slot, 2].astype(F32)
        eturn = pltpu.roll(emode, 4, 0)
        eturn = jnp.where(half, eturn, -eturn)
        bturn = pltpu.roll(bmode, 4, 0)
        bturn = jnp.where(half, bturn, -bturn)
        for side in range(2):
            if side == 0:
                weights = (lower_part, upper_part)
                turned = weights
            else:
                weights = (lower_part * column_sign, upper_part * upper_sign)
                turned = (-weights[0], -weights[1])

            def rows(values, scales):
                return jnp.concatenate([values * scales[0], values * scales[1]], axis=0).astype(BF16)

            minus = (-weights[0], -weights[1])
            straight = (-turned[0], -turned[1])
            base = side * 32
            pack_ref[slot, base : base + 16, 0:width] = rows(emode, minus)
            pack_ref[slot, base : base + 16, width : 2 * width] = rows(bturn, turned)
            pack_ref[slot, base + 16 : base + 32, 0:width] = rows(bmode, minus)
            pack_ref[slot, base + 16 : base + 32, width : 2 * width] = rows(eturn, straight)
            pack_ref[slot, 64 + side * 16 : 80 + side * 16, 0:width] = rows(temp, weights)
        both = lax.dot_general(
            leg_ref[1, slot], pack_ref[slot, 0:64, 0:width], NT, preferred_element_type=F32
        ) + lax.dot_general(
            leg_ref[2, slot], pack_ref[slot, 0:64, width : 2 * width], NT, preferred_element_type=F32
        )
        plain = lax.dot_general(
            leg_ref[0, slot], pack_ref[slot, 64:96, 0:width], NT, preferred_element_type=F32
        )
        lanes = slice(16 * slot, 16 * slot + 16)
        for side in range(2):
            acc_ref[side * 3, :, lanes] = plain[:, 16 * side : 16 * side + 16]
            acc_ref[side * 3 + 1, :, lanes] = both[:, 32 * side : 32 * side + 16]
            acc_ref[side * 3 + 2, :, lanes] = both[:, 32 * side + 16 : 32 * side + 32]
    for side in range(2):
        for field in range(3):
            start = side * pairs * 12 + field * 4 + group
            out_ref[pl.ds(start, pairs, stride=12), :] = acc_ref[side * 3 + field]


def legendre_sums(legendre, harmonics, orders):
    slots, pairs, width = legendre.shape[1:]
    return pl.pallas_call(
        legendre_kernel,
        grid_spec=pltpu.PrefetchScalarGridSpec(
            num_scalar_prefetch=1,
            grid=(slots // 8,),
            in_specs=[
                pl.BlockSpec((3, 8, pairs, width), lambda g, o: (0, g, 0, 0)),
                pl.BlockSpec((8, 3, 8, width), lambda g, o: (g, 0, 0, 0)),
            ],
            out_specs=pl.BlockSpec((2 * pairs * 12, 128), lambda g, o: (0, 0)),
            scratch_shapes=[
                pltpu.VMEM((8, 96, 2 * width), BF16),
                pltpu.VMEM((6, pairs, 128), F32),
            ],
        ),
        out_shape=jax.ShapeDtypeStruct((2 * pairs * 12, 128), F32),
        name="legendre_sums",
    )(orders, legendre, harmonics)


def cos_sin(phase):
    quarter = (phase + 2048) >> 12
    x = (phase - (quarter << 12)).astype(F32) * (math.pi / 8192)
    y = x * x
    sine = x + x * y * (-1.6666667e-1 + y * (8.3333310e-3 + y * (-1.9840874e-4 + y * 2.7525562e-6)))
    cosine = 1.0 + y * (-0.5 + y * (4.16666642e-2 + y * (-1.38887875e-3 + y * 2.4760495e-5)))
    swap = (quarter & 1) == 1
    cos_out = jnp.where(swap, sine, cosine)
    sin_out = jnp.where(swap, cosine, sine)
    cos_flip = ((quarter + 1) & 2) == 2
    sin_flip = (quarter & 2) == 2
    return jnp.where(cos_flip, -cos_out, cos_out), jnp.where(sin_flip, -sin_out, sin_out)


def high_low(value):
    high = value.astype(BF16)
    return high, (value - high.astype(F32)).astype(BF16)


def tables_kernel(shift_ref, lower_ref, high_ref, low_ref, cos_ref, sin_ref):
    slots = high_ref.shape[2] // 2
    tiles = slots // 128
    row = lax.broadcasted_iota(jnp.int32, (16, 128), 0)

    @pl.loop(0, tiles)
    def _(tile):
        lower = lower_ref[pl.ds(tile, 1), :]
        odd = lower % 2
        lanes = pl.multiple_of(tile * 128, 128)
        for parity in range(2):
            order = jnp.where(odd == parity, lower, 4095 - lower)
            factor = jnp.where(order == 0, 1.0, 2.0).astype(F32)
            cosine, sine = cos_sin((order * (512 * row + shift_ref[0])) & 16383)
            cos_ref[parity, tile] = cosine * factor
            sin_ref[parity, tile] = sine * factor
            cos_v, sin_v = cos_sin((order * (2 * row)) & 16383)
            cos_u, sin_u = cos_sin((order * (32 * row)) & 16383)
            for u in range(16):
                cu = cos_u[u : u + 1, :]
                su = sin_u[u : u + 1, :]
                pixels = slice(16 * u, 16 * u + 16)
                high, low = high_low(cu * cos_v - su * sin_v)
                high_ref[parity, pixels, pl.ds(lanes, 128)] = high
                low_ref[parity, pixels, pl.ds(lanes, 128)] = low
                high, low = high_low(su * cos_v + cu * sin_v)
                high_ref[parity, pixels, pl.ds(slots + lanes, 128)] = high
                low_ref[parity, pixels, pl.ds(slots + lanes, 128)] = low


def tables(shift, lower, slots):
    vmem = pl.BlockSpec(memory_space=pltpu.VMEM)
    return pl.pallas_call(
        tables_kernel,
        in_specs=[pl.BlockSpec(memory_space=pltpu.SMEM), vmem],
        out_specs=[vmem] * 4,
        out_shape=[
            jax.ShapeDtypeStruct((2, 256, 2 * slots), BF16),
            jax.ShapeDtypeStruct((2, 256, 2 * slots), BF16),
            jax.ShapeDtypeStruct((2, slots // 128, 16, 128), F32),
            jax.ShapeDtypeStruct((2, slots // 128, 16, 128), F32),
        ],
        name="tables",
    )(shift, lower)


def synthesis_kernel(lower_ref, cos_ref, sin_ref, high_ref, low_ref, sums_ref, out_ref, x_ref, a_ref):
    slots = high_ref.shape[2] // 2
    tiles = slots // 128
    for field in range(3):
        for pair in range(2):
            first = sums_ref[pl.ds(field * 4 + pair * 2, 64, stride=12), :]
            second = sums_ref[pl.ds(field * 4 + pair * 2 + 1, 64, stride=12), :]
            turned = jnp.concatenate([first, second], axis=0).T
            x_ref[field, pair * 8 : pair * 8 + 8] = turned.reshape(8, 16, 128)

    @pl.loop(0, tiles)
    def _(tile):
        odd = (lower_ref[pl.ds(tile, 1), :] % 2) == 1
        lanes = pl.multiple_of(tile * 128, 128)
        for field in range(3):
            x = x_ref[field, tile]
            for parity in range(2):
                keep = odd if parity else jnp.logical_not(odd)
                chosen = jnp.where(keep, x[0:8], x[8:16])
                cosine = cos_ref[parity, tile]
                sine = sin_ref[parity, tile]
                for comp in range(4):
                    real = chosen[comp : comp + 1, :]
                    imag = chosen[4 + comp : 5 + comp, :]
                    rows = (field * 4 + comp) * 16
                    high, low = high_low(real * cosine - imag * sine)
                    a_ref[parity, rows : rows + 16, pl.ds(lanes, 128)] = high
                    a_ref[parity, 192 + rows : 208 + rows, pl.ds(lanes, 128)] = low
                    high, low = high_low(-(real * sine + imag * cosine))
                    a_ref[parity, rows : rows + 16, pl.ds(slots + lanes, 128)] = high
                    a_ref[parity, 192 + rows : 208 + rows, pl.ds(slots + lanes, 128)] = low

    parts = []
    for parity in range(2):
        wide = lax.dot_general(a_ref[parity], high_ref[parity], NT, preferred_element_type=F32)
        fine = lax.dot_general(a_ref[parity, 0:192, :], low_ref[parity], NT, preferred_element_type=F32)
        parts.append(wide[0:192] + (wide[192:384] + fine))
    near = parts[0] + parts[1]
    far = parts[0] - parts[1]
    for block in range(4):
        for row in range(12):
            place = slice(row * 4, row * 4 + 4)
            source = slice(row * 16 + block * 4, row * 16 + block * 4 + 4)
            out_ref[block, place, :] = near[source, :]
            out_ref[block + 4, place, :] = far[source, :]


def synthesis(lower, cosine, sine, high, low, sums):
    vmem = pl.BlockSpec(memory_space=pltpu.VMEM)
    slots = high.shape[2] // 2
    return pl.pallas_call(
        synthesis_kernel,
        in_specs=[vmem] * 6,
        out_specs=vmem,
        out_shape=jax.ShapeDtypeStruct((8, 48, 256), F32),
        scratch_shapes=[
            pltpu.VMEM((3, slots // 128, 16, 128), F32),
            pltpu.VMEM((2, 384, 2 * slots), BF16),
        ],
        name="synthesis",
    )(lower, cosine, sine, high, low, sums)


def total_kernel(parts_ref, out_ref, sum_ref):
    total = parts_ref[0]
    for source in range(1, 8):
        total = total + parts_ref[source]
    sum_ref[0] = total[:, 0:128]
    sum_ref[1] = total[:, 128:256]
    for field in range(3):
        for piece in range(4):
            for side in range(2):
                start = piece * 256 + side * 128
                out_ref[0, field, :, start : start + 128] = sum_ref[side, pl.ds(field * 16 + piece, 4, stride=4), :]


def total(parts):
    vmem = pl.BlockSpec(memory_space=pltpu.VMEM)
    return pl.pallas_call(
        total_kernel,
        in_specs=[vmem],
        out_specs=vmem,
        out_shape=jax.ShapeDtypeStruct((1, 3, 4, 1024), F32),
        scratch_shapes=[pltpu.VMEM((2, 48, 128), F32)],
        name="total",
    )(parts)


def body(legendre, harmonics, slot_orders, cycle_index):
    slots_here = harmonics.shape[0]
    columns_here = harmonics.shape[-1]
    slots = slot_orders.shape[0]
    pairs = cycle_index.shape[0]
    place = lax.axis_index("ma")
    lower_here = lax.dynamic_slice_in_dim(slot_orders, place * slots_here, slots_here)
    first_column = lax.axis_index("ell") * columns_here
    orders = jnp.concatenate([jnp.stack([jnp.int32(2 * slots), first_column.astype(jnp.int32)]), lower_here])
    sums = legendre_sums(legendre, harmonics.reshape(slots_here, 3, 8, columns_here), orders)
    moved = lax.all_to_all(sums.reshape(64, 3, 4, 128), "ma", split_axis=0, concat_axis=0, tiled=True)
    shift = lax.dynamic_slice_in_dim(cycle_index, place % pairs, 1) % 2
    lower = slot_orders.reshape(64, 2, 2, 8).transpose(1, 3, 2, 0).reshape(16, 128)
    high, low, cosine, sine = tables(shift, lower, slots)
    blocks = synthesis(lower, cosine, sine, high, low, moved.reshape(768, 128))
    arrived = lax.all_to_all(blocks, "ell", split_axis=0, concat_axis=0, tiled=True)
    return total(arrived)


def solution(mesh):
    return jax.shard_map(
        body,
        mesh=mesh,
        in_specs=(P(None, "ma", None, "ell"), P("ma", None, None, None, "ell"), P(), P()),
        out_specs=P("ma", None, None, "ell"),
        check_vma=False,
    )
```

```python
import math

import jax
import jax.numpy as jnp
from jax import lax
from jax.experimental import pallas as pl
from jax.experimental.pallas import tpu as pltpu
from jax.sharding import PartitionSpec as P

F32 = jnp.float32
BF16 = jnp.bfloat16
NT = (((1,), (1,)), ((), ()))


def legendre_kernel(orders_ref, leg_ref, harm_ref, out_ref, pack_ref, acc_ref):
    group = pl.program_id(0)
    groups = pl.num_programs(0)
    pairs = leg_ref.shape[2]
    width = leg_ref.shape[3]
    full = 2 * orders_ref.shape[0]
    first_slot = lax.axis_index("ma") * (8 * groups) + group * 8
    column = lax.axis_index("ell") * width + lax.broadcasted_iota(jnp.int32, (1, width), 1)
    column_sign = (1 - 2 * (column % 2)).astype(F32)
    half = lax.broadcasted_iota(jnp.int32, (8, width), 0) < 4
    for slot in range(8):
        lower = orders_ref[first_slot + slot]
        boundary = full - 1 - lower
        lower_part = jnp.where(column < boundary, 1.0, 0.0).astype(F32)
        upper_part = jnp.where((column >= boundary) & (column < full - 1), 1.0, 0.0).astype(F32)
        upper_sign = column_sign * (2 * (lower % 2) - 1).astype(F32)
        temp, emode, bmode = (
            jnp.concatenate([harm_ref[slot, kind, part].astype(F32) for part in range(2)], axis=0)
            for kind in range(3)
        )
        eturn = pltpu.roll(emode, 4, 0)
        eturn = jnp.where(half, eturn, -eturn)
        bturn = pltpu.roll(bmode, 4, 0)
        bturn = jnp.where(half, bturn, -bturn)
        for side in range(2):
            if side == 0:
                weights = (lower_part, upper_part)
                turned = weights
            else:
                weights = (lower_part * column_sign, upper_part * upper_sign)
                turned = (-weights[0], -weights[1])

            def rows(values, scales):
                return jnp.concatenate([values * scales[0], values * scales[1]], axis=0).astype(BF16)

            minus = (-weights[0], -weights[1])
            straight = (-turned[0], -turned[1])
            base = side * 32
            pack_ref[slot, base : base + 16, 0:width] = rows(emode, minus)
            pack_ref[slot, base : base + 16, width : 2 * width] = rows(bturn, turned)
            pack_ref[slot, base + 16 : base + 32, 0:width] = rows(bmode, minus)
            pack_ref[slot, base + 16 : base + 32, width : 2 * width] = rows(eturn, straight)
            pack_ref[slot, 64 + side * 16 : 80 + side * 16, 0:width] = rows(temp, weights)
        both = lax.dot_general(
            leg_ref[1, slot], pack_ref[slot, 0:64, 0:width], NT, preferred_element_type=F32
        ) + lax.dot_general(
            leg_ref[2, slot], pack_ref[slot, 0:64, width : 2 * width], NT, preferred_element_type=F32
        )
        plain = lax.dot_general(
            leg_ref[0, slot], pack_ref[slot, 64:96, 0:width], NT, preferred_element_type=F32
        )
        lanes = slice(16 * slot, 16 * slot + 16)
        for side in range(2):
            acc_ref[side * 3, :, lanes] = plain[:, 16 * side : 16 * side + 16]
            acc_ref[side * 3 + 1, :, lanes] = both[:, 32 * side : 32 * side + 16]
            acc_ref[side * 3 + 2, :, lanes] = both[:, 32 * side + 16 : 32 * side + 32]
    for side in range(2):
        for field in range(3):
            start = side * pairs * 12 + field * 4 + group
            out_ref[pl.ds(start, pairs, stride=12), :] = acc_ref[side * 3 + field]


def legendre_sums(legendre, harmonics, orders):
    slots, pairs, width = legendre.shape[1:]
    return pl.pallas_call(
        legendre_kernel,
        grid_spec=pltpu.PrefetchScalarGridSpec(
            num_scalar_prefetch=1,
            grid=(slots // 8,),
            in_specs=[
                pl.BlockSpec((3, 8, pairs, width), lambda g, o: (0, g, 0, 0)),
                pl.BlockSpec((8, 3, 2, 4, width), lambda g, o: (g, 0, 0, 0, 0)),
            ],
            out_specs=pl.BlockSpec((2 * pairs * 12, 128), lambda g, o: (0, 0)),
            scratch_shapes=[
                pltpu.VMEM((8, 96, 2 * width), BF16),
                pltpu.VMEM((6, pairs, 128), F32),
            ],
        ),
        out_shape=jax.ShapeDtypeStruct((2 * pairs * 12, 128), F32),
        name="legendre_sums",
    )(orders, legendre, harmonics)


def cos_sin(phase):
    quarter = (phase + 2048) >> 12
    x = (phase - (quarter << 12)).astype(F32) * (math.pi / 8192)
    y = x * x
    sine = x + x * y * (-1.6666667e-1 + y * (8.3333310e-3 + y * (-1.9840874e-4 + y * 2.7525562e-6)))
    cosine = 1.0 + y * (-0.5 + y * (4.16666642e-2 + y * (-1.38887875e-3 + y * 2.4760495e-5)))
    swap = (quarter & 1) == 1
    cos_out = jnp.where(swap, sine, cosine)
    sin_out = jnp.where(swap, cosine, sine)
    cos_flip = ((quarter + 1) & 2) == 2
    sin_flip = (quarter & 2) == 2
    return jnp.where(cos_flip, -cos_out, cos_out), jnp.where(sin_flip, -sin_out, sin_out)


def high_low(value):
    high = value.astype(BF16)
    return high, (value - high.astype(F32)).astype(BF16)


def tables_kernel(cycle_ref, slots_ref, lower_ref, cos_ref, sin_ref, high_ref, low_ref, high_buf, low_buf, sem):
    slots = high_ref.shape[2] // 2
    tiles = slots // 128
    shift = cycle_ref[lax.axis_index("ma") % cycle_ref.shape[0]] % 2
    row = lax.broadcasted_iota(jnp.int32, (16, 128), 0)
    turned = slots_ref[...].astype(F32).T
    pieces = []
    for middle in range(2):
        for device in range(4):
            start = device * 32 + middle * 8
            pieces.append(
                jnp.concatenate([turned[start : start + 8], turned[start + 16 : start + 24]], axis=0)
            )
    lower_ref[...] = jnp.concatenate(pieces, axis=1).astype(jnp.int32)

    def one_tile(tile):
        lower = lower_ref[pl.ds(tile, 1), :]
        odd = lower % 2
        lanes = pl.multiple_of(tile * 128, 128)
        for parity in range(2):
            order = jnp.where(odd == parity, lower, 4095 - lower)
            factor = jnp.where(order == 0, 1.0, 2.0).astype(F32)
            cosine, sine = cos_sin((order * (512 * row + shift)) & 16383)
            cos_ref[parity, tile] = cosine * factor
            sin_ref[parity, tile] = sine * factor
            cos_v, sin_v = cos_sin((order * (2 * row)) & 16383)
            cos_u, sin_u = cos_sin((order * (32 * row)) & 16383)
            for u in range(16):
                cu = cos_u[u : u + 1, :]
                su = sin_u[u : u + 1, :]
                pixels = slice(16 * u, 16 * u + 16)
                high, low = high_low(cu * cos_v - su * sin_v)
                high_buf[parity, pixels, pl.ds(lanes, 128)] = high
                low_buf[parity, pixels, pl.ds(lanes, 128)] = low
                high, low = high_low(su * cos_v + cu * sin_v)
                high_buf[parity, pixels, pl.ds(slots + lanes, 128)] = high
                low_buf[parity, pixels, pl.ds(slots + lanes, 128)] = low

    copies = []
    span = 4
    for block in range(tiles // span):
        pl.loop(block * span, (block + 1) * span)(one_tile)
        for parity in range(2):
            for part in range(2):
                for buf, ref in ((high_buf, high_ref), (low_buf, low_ref)):
                    view = (parity, slice(None), pl.ds(part * slots + block * span * 128, span * 128))
                    copy = pltpu.make_async_copy(buf.at[view], ref.at[view], sem.at[len(copies)])
                    copy.start()
                    copies.append(copy)
    for copy in copies:
        copy.wait()


def tables(cycle_index, slot_orders):
    slots = slot_orders.shape[0]
    vmem = pl.BlockSpec(memory_space=pltpu.VMEM)
    hbm = pl.BlockSpec(memory_space=pltpu.HBM)
    small = jax.ShapeDtypeStruct((2, slots // 128, 16, 128), F32)
    large = jax.ShapeDtypeStruct((2, 256, 2 * slots), BF16)
    return pl.pallas_call(
        tables_kernel,
        in_specs=[pl.BlockSpec(memory_space=pltpu.SMEM), vmem],
        out_specs=[vmem, vmem, vmem, hbm, hbm],
        out_shape=[jax.ShapeDtypeStruct((slots // 128, 128), jnp.int32), small, small, large, large],
        scratch_shapes=[
            pltpu.VMEM((2, 256, 2 * slots), BF16),
            pltpu.VMEM((2, 256, 2 * slots), BF16),
            pltpu.SemaphoreType.DMA((slots // 64,)),
        ],
        compiler_params=pltpu.CompilerParams(vmem_limit_bytes=60 << 20),
        name="tables",
    )(cycle_index, slot_orders.reshape(slots // 128, 128))


def synthesis_kernel(
    lower_ref, cos_ref, sin_ref, high_ref, low_ref, sums_ref, out_ref, x_ref, a_ref, high_buf, low_buf, sem
):
    slots = high_ref.shape[2] // 2
    tiles = slots // 128
    copies = [
        [
            pltpu.make_async_copy(ref.at[parity], buf.at[parity], sem.at[2 * parity + i])
            for i, (ref, buf) in enumerate(((high_ref, high_buf), (low_ref, low_buf)))
        ]
        for parity in range(2)
    ]
    for pair in copies:
        for copy in pair:
            copy.start()
    for field in range(3):
        for pair in range(2):
            pieces = []
            for middle in range(2):
                for device in range(4):
                    start = device * 12 + field * 4 + pair * 2 + middle
                    pieces.append(sums_ref[pl.ds(start, 16, stride=48), :])
            turned = jnp.concatenate(pieces, axis=0).T
            x_ref[field, pair * 8 : pair * 8 + 8] = turned.reshape(8, 16, 128)

    @pl.loop(0, tiles)
    def _(tile):
        odd = (lower_ref[pl.ds(tile, 1), :] % 2) == 1
        lanes = pl.multiple_of(tile * 128, 128)
        for field in range(3):
            x = x_ref[field, tile]
            for parity in range(2):
                keep = odd if parity else jnp.logical_not(odd)
                chosen = jnp.where(keep, x[0:8], x[8:16])
                cosine = cos_ref[parity, tile]
                sine = sin_ref[parity, tile]
                for comp in range(4):
                    real = chosen[comp : comp + 1, :]
                    imag = chosen[4 + comp : 5 + comp, :]
                    rows = (field * 4 + comp) * 16
                    high, low = high_low(real * cosine - imag * sine)
                    a_ref[parity, rows : rows + 16, pl.ds(lanes, 128)] = high
                    a_ref[parity, 192 + rows : 208 + rows, pl.ds(lanes, 128)] = low
                    high, low = high_low(-(real * sine + imag * cosine))
                    a_ref[parity, rows : rows + 16, pl.ds(slots + lanes, 128)] = high
                    a_ref[parity, 192 + rows : 208 + rows, pl.ds(slots + lanes, 128)] = low

    parts = []
    for parity in range(2):
        for copy in copies[parity]:
            copy.wait()
        wide = lax.dot_general(a_ref[parity], high_buf[parity], NT, preferred_element_type=F32)
        fine = lax.dot_general(a_ref[parity, 0:192, :], low_buf[parity], NT, preferred_element_type=F32)
        parts.append(wide[0:192] + (wide[192:384] + fine))
    near = parts[0] + parts[1]
    far = parts[0] - parts[1]
    for block in range(4):
        for row in range(12):
            place = slice(row * 4, row * 4 + 4)
            source = slice(row * 16 + block * 4, row * 16 + block * 4 + 4)
            out_ref[block, place, :] = near[source, :]
            out_ref[block + 4, place, :] = far[source, :]


def synthesis(lower, cosine, sine, high, low, sums):
    vmem = pl.BlockSpec(memory_space=pltpu.VMEM)
    hbm = pl.BlockSpec(memory_space=pltpu.HBM)
    slots = high.shape[2] // 2
    return pl.pallas_call(
        synthesis_kernel,
        in_specs=[vmem, vmem, vmem, hbm, hbm, vmem],
        out_specs=vmem,
        out_shape=jax.ShapeDtypeStruct((8, 48, 256), F32),
        scratch_shapes=[
            pltpu.VMEM((3, slots // 128, 16, 128), F32),
            pltpu.VMEM((2, 384, 2 * slots), BF16),
            pltpu.VMEM((2, 256, 2 * slots), BF16),
            pltpu.VMEM((2, 256, 2 * slots), BF16),
            pltpu.SemaphoreType.DMA((4,)),
        ],
        compiler_params=pltpu.CompilerParams(vmem_limit_bytes=60 << 20),
        name="synthesis",
    )(lower, cosine, sine, high, low, sums)


def total_kernel(parts_ref, out_ref, sum_ref):
    total = parts_ref[0]
    for source in range(1, 8):
        total = total + parts_ref[source]
    sum_ref[0] = total[:, 0:128]
    sum_ref[1] = total[:, 128:256]
    for field in range(3):
        for piece in range(4):
            for side in range(2):
                start = piece * 256 + side * 128
                out_ref[0, field, :, start : start + 128] = sum_ref[side, pl.ds(field * 16 + piece, 4, stride=4), :]


def total(parts):
    vmem = pl.BlockSpec(memory_space=pltpu.VMEM)
    return pl.pallas_call(
        total_kernel,
        in_specs=[vmem],
        out_specs=vmem,
        out_shape=jax.ShapeDtypeStruct((1, 3, 4, 1024), F32),
        scratch_shapes=[pltpu.VMEM((2, 48, 128), F32)],
        compiler_params=pltpu.CompilerParams(vmem_limit_bytes=8 << 20),
        name="total",
    )(parts)


def body(legendre, harmonics, slot_orders, cycle_index):
    sums = legendre_sums(legendre, harmonics, slot_orders)
    moved = lax.all_to_all(sums.reshape(64, 3, 4, 128), "ma", split_axis=0, concat_axis=0, tiled=True)
    lower, cosine, sine, high, low = tables(cycle_index, slot_orders)
    blocks = synthesis(lower, cosine, sine, high, low, moved.reshape(768, 128))
    arrived = lax.all_to_all(blocks, "ell", split_axis=0, concat_axis=0, tiled=True)
    return total(arrived)


def solution(mesh):
    return jax.shard_map(
        body,
        mesh=mesh,
        in_specs=(P(None, "ma", None, "ell"), P("ma", None, None, None, "ell"), P(), P()),
        out_specs=P("ma", None, None, "ell"),
        check_vma=False,
    )
```

```python
import math

import jax
import jax.numpy as jnp
from jax import lax
from jax.experimental import pallas as pl
from jax.experimental.pallas import tpu as pltpu
from jax.sharding import PartitionSpec as P

F32 = jnp.float32
BF16 = jnp.bfloat16
NT = (((1,), (1,)), ((), ()))


def legendre_kernel(orders_ref, leg_ref, harm_ref, out_ref, pack_ref, acc_ref):
    group = pl.program_id(0)
    groups = pl.num_programs(0)
    pairs = leg_ref.shape[2]
    width = leg_ref.shape[3]
    full = 2 * orders_ref.shape[0]
    first_slot = lax.axis_index("ma") * (8 * groups) + group * 8
    column = lax.axis_index("ell") * width + lax.broadcasted_iota(jnp.int32, (1, width), 1)
    column_sign = (1 - 2 * (column % 2)).astype(F32)
    half = lax.broadcasted_iota(jnp.int32, (8, width), 0) < 4
    for slot in range(8):
        lower = orders_ref[first_slot + slot]
        boundary = full - 1 - lower
        lower_part = jnp.where(column < boundary, 1.0, 0.0).astype(F32)
        upper_part = jnp.where((column >= boundary) & (column < full - 1), 1.0, 0.0).astype(F32)
        upper_sign = column_sign * (2 * (lower % 2) - 1).astype(F32)
        temp, emode, bmode = (
            jnp.concatenate([harm_ref[slot, kind, part].astype(F32) for part in range(2)], axis=0)
            for kind in range(3)
        )
        eturn = pltpu.roll(emode, 4, 0)
        eturn = jnp.where(half, eturn, -eturn)
        bturn = pltpu.roll(bmode, 4, 0)
        bturn = jnp.where(half, bturn, -bturn)
        for side in range(2):
            if side == 0:
                weights = (lower_part, upper_part)
                turned = weights
            else:
                weights = (lower_part * column_sign, upper_part * upper_sign)
                turned = (-weights[0], -weights[1])

            def rows(values, scales):
                return jnp.concatenate([values * scales[0], values * scales[1]], axis=0).astype(BF16)

            minus = (-weights[0], -weights[1])
            straight = (-turned[0], -turned[1])
            base = side * 32
            pack_ref[slot, base : base + 16, 0:width] = rows(emode, minus)
            pack_ref[slot, base : base + 16, width : 2 * width] = rows(bturn, turned)
            pack_ref[slot, base + 16 : base + 32, 0:width] = rows(bmode, minus)
            pack_ref[slot, base + 16 : base + 32, width : 2 * width] = rows(eturn, straight)
            pack_ref[slot, 64 + side * 16 : 80 + side * 16, 0:width] = rows(temp, weights)
        both = lax.dot_general(
            leg_ref[1, slot], pack_ref[slot, 0:64, 0:width], NT, preferred_element_type=F32
        ) + lax.dot_general(
            leg_ref[2, slot], pack_ref[slot, 0:64, width : 2 * width], NT, preferred_element_type=F32
        )
        plain = lax.dot_general(
            leg_ref[0, slot], pack_ref[slot, 64:96, 0:width], NT, preferred_element_type=F32
        )
        lanes = slice(16 * slot, 16 * slot + 16)
        for side in range(2):
            acc_ref[side * 3, :, lanes] = plain[:, 16 * side : 16 * side + 16]
            acc_ref[side * 3 + 1, :, lanes] = both[:, 32 * side : 32 * side + 16]
            acc_ref[side * 3 + 2, :, lanes] = both[:, 32 * side + 16 : 32 * side + 32]
    for side in range(2):
        for field in range(3):
            start = side * pairs * 12 + field * 4 + group
            out_ref[pl.ds(start, pairs, stride=12), :] = acc_ref[side * 3 + field]


def legendre_sums(legendre, harmonics, orders):
    slots, pairs, width = legendre.shape[1:]
    return pl.pallas_call(
        legendre_kernel,
        grid=(slots // 8,),
        in_specs=[
            pl.BlockSpec(memory_space=pltpu.SMEM),
            pl.BlockSpec((3, 8, pairs, width), lambda g: (0, g, 0, 0)),
            pl.BlockSpec((8, 3, 2, 4, width), lambda g: (g, 0, 0, 0, 0)),
        ],
        out_specs=pl.BlockSpec((2 * pairs * 12, 128), lambda g: (0, 0)),
        scratch_shapes=[
            pltpu.VMEM((8, 96, 2 * width), BF16),
            pltpu.VMEM((6, pairs, 128), F32),
        ],
        out_shape=jax.ShapeDtypeStruct((2 * pairs * 12, 128), F32),
        name="legendre_sums",
    )(orders, legendre, harmonics)


def cos_sin(phase):
    quarter = (phase + 2048) >> 12
    x = (phase - (quarter << 12)).astype(F32) * (math.pi / 8192)
    y = x * x
    sine = x + x * y * (-1.6666667e-1 + y * (8.3333310e-3 + y * (-1.9840874e-4 + y * 2.7525562e-6)))
    cosine = 1.0 + y * (-0.5 + y * (4.16666642e-2 + y * (-1.38887875e-3 + y * 2.4760495e-5)))
    swap = (quarter & 1) == 1
    cos_out = jnp.where(swap, sine, cosine)
    sin_out = jnp.where(swap, cosine, sine)
    cos_flip = ((quarter + 1) & 2) == 2
    sin_flip = (quarter & 2) == 2
    return jnp.where(cos_flip, -cos_out, cos_out), jnp.where(sin_flip, -sin_out, sin_out)


def high_low(value):
    high = value.astype(BF16)
    return high, (value - high.astype(F32)).astype(BF16)


def tables_kernel(cycle_ref, slots_ref, lower_ref, cos_ref, sin_ref, table_ref, table_buf, sem):
    slots = table_ref.shape[3]
    tiles = slots // 128
    shift = cycle_ref[lax.axis_index("ma") % cycle_ref.shape[0]] % 2
    row = lax.broadcasted_iota(jnp.int32, (16, 128), 0)
    turned = slots_ref[...].astype(F32).T
    pieces = []
    for middle in range(2):
        for device in range(4):
            start = device * 32 + middle * 8
            pieces.append(
                jnp.concatenate([turned[start : start + 8], turned[start + 16 : start + 24]], axis=0)
            )
    lower_ref[...] = jnp.concatenate(pieces, axis=1).astype(jnp.int32)

    def one_tile(tile):
        lower = lower_ref[pl.ds(tile, 1), :]
        odd = lower % 2
        lanes = pl.ds(pl.multiple_of(tile * 128, 128), 128)
        for parity in range(2):
            order = jnp.where(odd == parity, lower, 4095 - lower)
            factor = jnp.where(order == 0, 1.0, 2.0).astype(F32)
            cosine, sine = cos_sin((order * (512 * row + (255 + shift))) & 16383)
            cos_ref[parity, tile] = cosine * factor
            sin_ref[parity, tile] = sine * factor
            cos_v, sin_v = cos_sin((order * (2 * row + 1)) & 16383)
            cos_u, sin_u = cos_sin((order * (32 * row[0:8])) & 16383)
            for u in range(8):
                cu = cos_u[u : u + 1, :]
                su = sin_u[u : u + 1, :]
                for part, value in enumerate((cu * cos_v - su * sin_v, su * cos_v + cu * sin_v)):
                    high, low = high_low(value)
                    table_buf[parity, part, 16 * u : 16 * u + 16, lanes] = high
                    table_buf[parity, part, 128 + 16 * u : 144 + 16 * u, lanes] = low

    copies = []
    span = 4
    for block in range(tiles // span):
        pl.loop(block * span, (block + 1) * span)(one_tile)
        for parity in range(2):
            for part in range(2):
                view = (parity, part, slice(None), pl.ds(block * span * 128, span * 128))
                copy = pltpu.make_async_copy(table_buf.at[view], table_ref.at[view], sem.at[len(copies)])
                copy.start()
                copies.append(copy)
    for copy in copies:
        copy.wait()


def tables(cycle_index, slot_orders):
    slots = slot_orders.shape[0]
    vmem = pl.BlockSpec(memory_space=pltpu.VMEM)
    hbm = pl.BlockSpec(memory_space=pltpu.HBM)
    small = jax.ShapeDtypeStruct((2, slots // 128, 16, 128), F32)
    return pl.pallas_call(
        tables_kernel,
        in_specs=[pl.BlockSpec(memory_space=pltpu.SMEM), vmem],
        out_specs=[vmem, vmem, vmem, hbm],
        out_shape=[
            jax.ShapeDtypeStruct((slots // 128, 128), jnp.int32),
            small,
            small,
            jax.ShapeDtypeStruct((2, 2, 256, slots), BF16),
        ],
        scratch_shapes=[
            pltpu.VMEM((2, 2, 256, slots), BF16),
            pltpu.SemaphoreType.DMA((slots // 128,)),
        ],
        compiler_params=pltpu.CompilerParams(vmem_limit_bytes=52 << 20),
        name="tables",
    )(cycle_index, slot_orders.reshape(slots // 128, 128))


def synthesis_kernel(lower_ref, cos_ref, sin_ref, table_ref, sums_ref, out_ref, x_ref, a_ref, table_buf, sem):
    slots = table_ref.shape[3]
    tiles = slots // 128
    copies = [
        pltpu.make_async_copy(table_ref.at[parity], table_buf.at[parity], sem.at[parity]) for parity in range(2)
    ]
    for copy in copies:
        copy.start()
    for field in range(3):
        for pair in range(2):
            pieces = []
            for middle in range(2):
                for device in range(4):
                    start = device * 12 + field * 4 + pair * 2 + middle
                    pieces.append(sums_ref[pl.ds(start, 16, stride=48), :])
            turned = jnp.concatenate(pieces, axis=0).T
            x_ref[field, pair * 8 : pair * 8 + 8] = turned.reshape(8, 16, 128)

    @pl.loop(0, tiles)
    def _(tile):
        odd = (lower_ref[pl.ds(tile, 1), :] % 2) == 1
        lanes = pl.ds(pl.multiple_of(tile * 128, 128), 128)
        for field in range(3):
            x = x_ref[field, tile]
            for parity in range(2):
                keep = odd if parity else jnp.logical_not(odd)
                chosen = jnp.where(keep, x[0:8], x[8:16])
                cosine = cos_ref[parity, tile]
                sine = sin_ref[parity, tile]
                for comp in range(4):
                    real = chosen[comp : comp + 1, :]
                    imag = chosen[4 + comp : 5 + comp, :]
                    rows = (field * 4 + comp) * 16
                    for part, value in enumerate(
                        (real * cosine - imag * sine, -(real * sine + imag * cosine))
                    ):
                        high, low = high_low(value)
                        a_ref[parity, part, rows : rows + 16, lanes] = high
                        a_ref[parity, part, 192 + rows : 208 + rows, lanes] = low

    sides = []
    for parity in range(2):
        copies[parity].wait()
        both = []
        for part in range(2):
            wide = lax.dot_general(
                a_ref[parity, part], table_buf[parity, part], NT, preferred_element_type=F32
            )
            fine = wide[0:192, 128:256] + wide[192:384, 128:256]
            both.append(wide[0:192, 0:128] + (wide[192:384, 0:128] + fine))
        sides.append((both[0] - both[1], both[0] + both[1]))
    for side in range(2):
        lanes = slice(side * 128, side * 128 + 128)
        near = sides[0][side] + sides[1][side]
        far = sides[0][side] - sides[1][side]
        for block in range(4):
            for row in range(12):
                place = slice(row * 4, row * 4 + 4)
                source = slice(row * 16 + block * 4, row * 16 + block * 4 + 4)
                out_ref[block, place, lanes] = near[source, :]
                out_ref[block + 4, place, lanes] = far[source, :]


def synthesis(lower, cosine, sine, table, sums):
    vmem = pl.BlockSpec(memory_space=pltpu.VMEM)
    hbm = pl.BlockSpec(memory_space=pltpu.HBM)
    slots = table.shape[3]
    return pl.pallas_call(
        synthesis_kernel,
        in_specs=[vmem, vmem, vmem, hbm, vmem],
        out_specs=vmem,
        out_shape=jax.ShapeDtypeStruct((8, 48, 256), F32),
        scratch_shapes=[
            pltpu.VMEM((3, slots // 128, 16, 128), F32),
            pltpu.VMEM((2, 2, 384, slots), BF16),
            pltpu.VMEM((2, 2, 256, slots), BF16),
            pltpu.SemaphoreType.DMA((2,)),
        ],
        compiler_params=pltpu.CompilerParams(vmem_limit_bytes=52 << 20),
        name="synthesis",
    )(lower, cosine, sine, table, sums)


def total_kernel(parts_ref, out_ref, sum_ref):
    total = parts_ref[0]
    for source in range(1, 8):
        total = total + parts_ref[source]
    falling = 127 - lax.broadcasted_iota(jnp.int32, (48, 128), 1)
    sum_ref[0] = jnp.take_along_axis(total[:, 0:128], falling, axis=1)
    sum_ref[1] = total[:, 128:256]
    for field in range(3):
        for piece in range(4):
            for side in range(2):
                start = piece * 256 + side * 128
                out_ref[0, field, :, start : start + 128] = sum_ref[side, pl.ds(field * 16 + piece, 4, stride=4), :]


def total(parts):
    vmem = pl.BlockSpec(memory_space=pltpu.VMEM)
    return pl.pallas_call(
        total_kernel,
        in_specs=[vmem],
        out_specs=vmem,
        out_shape=jax.ShapeDtypeStruct((1, 3, 4, 1024), F32),
        scratch_shapes=[pltpu.VMEM((2, 48, 128), F32)],
        compiler_params=pltpu.CompilerParams(vmem_limit_bytes=8 << 20),
        name="total",
    )(parts)


def body(legendre, harmonics, slot_orders, cycle_index):
    sums = legendre_sums(legendre, harmonics, slot_orders)
    moved = lax.all_to_all(sums.reshape(64, 3, 4, 128), "ma", split_axis=0, concat_axis=0, tiled=True)
    lower, cosine, sine, table = tables(cycle_index, slot_orders)
    blocks = synthesis(lower, cosine, sine, table, moved.reshape(768, 128))
    arrived = lax.all_to_all(blocks, "ell", split_axis=0, concat_axis=0, tiled=True)
    return total(arrived)


def solution(mesh):
    return jax.shard_map(
        body,
        mesh=mesh,
        in_specs=(P(None, "ma", None, "ell"), P("ma", None, None, None, "ell"), P(), P()),
        out_specs=P("ma", None, None, "ell"),
        check_vma=False,
    )
```

```python
import math

import jax
import jax.numpy as jnp
from jax import lax
from jax.experimental import pallas as pl
from jax.experimental.pallas import tpu as pltpu
from jax.sharding import PartitionSpec as P

F32 = jnp.float32
BF16 = jnp.bfloat16
NT = (((1,), (1,)), ((), ()))


def legendre_kernel(
    orders_hbm, leg_hbm, harm_hbm, out_ref, orders_ref, leg_all, harm_all, pack_ref, acc_ref, sem, orders_sem
):
    groups = leg_hbm.shape[1] // 8
    orders_copy = pltpu.make_async_copy(orders_hbm, orders_ref, orders_sem)
    orders_copy.start()

    def arrivals(group):
        span = pl.ds(group * 8, 8)
        return (
            pltpu.make_async_copy(harm_hbm.at[span], harm_all.at[span], sem.at[0, group]),
            pltpu.make_async_copy(leg_hbm.at[:, span], leg_all.at[:, span], sem.at[1, group]),
        )

    for group in range(groups):
        for copy in arrivals(group):
            copy.start()
    orders_copy.wait()

    @pl.loop(0, groups)
    def _(group):
        for copy in arrivals(group):
            copy.wait()
        span = pl.ds(group * 8, 8)
        legendre_group(
            group, groups, orders_ref, leg_all.at[:, span], harm_all.at[span], out_ref, pack_ref, acc_ref
        )


def legendre_group(group, groups, orders_ref, leg_ref, harm_ref, out_ref, pack_ref, acc_ref):
    pairs = leg_ref.shape[2]
    width = leg_ref.shape[3]
    full = 2 * orders_ref.shape[0]
    first_slot = lax.axis_index("ma") * (8 * groups) + group * 8
    column = lax.axis_index("ell") * width + lax.broadcasted_iota(jnp.int32, (1, width), 1)
    column_sign = (1 - 2 * (column % 2)).astype(F32)
    half = lax.broadcasted_iota(jnp.int32, (8, width), 0) < 4
    upper_rows = lax.broadcasted_iota(jnp.int32, (16, width), 0) >= 8
    for slot in range(8):
        lower = orders_ref[first_slot + slot]
        boundary = full - 1 - lower
        past = column >= boundary
        inside = (column < full - 1) & (past == upper_rows)
        weights = jnp.where(inside, 1.0, 0.0).astype(F32)
        flips = column_sign * jnp.where(upper_rows, (2 * (lower % 2) - 1).astype(F32), 1.0)
        signed = weights * flips
        temp, emode, bmode = (
            jnp.concatenate([harm_ref[slot, kind, part].astype(F32) for part in range(2)], axis=0)
            for kind in range(3)
        )
        eturn = pltpu.roll(emode, 4, 0)
        eturn = jnp.where(half, -eturn, eturn)
        bturn = pltpu.roll(bmode, 4, 0)
        bturn = jnp.where(half, bturn, -bturn)

        def twice(values):
            return jnp.concatenate([values, values], axis=0).astype(BF16)

        temp, emode, bmode = twice(temp), twice(-emode), twice(-bmode)
        eturn, bturn = twice(eturn), twice(bturn)
        for side in range(2):
            straight = (signed if side else weights).astype(BF16)
            turned = (-signed).astype(BF16) if side else straight
            base = side * 32
            pack_ref[slot, base : base + 16, 0:width] = emode * straight
            pack_ref[slot, base : base + 16, width : 2 * width] = bturn * turned
            pack_ref[slot, base + 16 : base + 32, 0:width] = bmode * straight
            pack_ref[slot, base + 16 : base + 32, width : 2 * width] = eturn * turned
            pack_ref[slot, 64 + side * 16 : 80 + side * 16, 0:width] = temp * straight
        both = lax.dot_general(
            jnp.concatenate([leg_ref[1, slot], leg_ref[2, slot]], axis=1),
            pack_ref[slot, 0:64],
            NT,
            preferred_element_type=F32,
        )
        plain = lax.dot_general(
            leg_ref[0, slot], pack_ref[slot, 64:96, 0:width], NT, preferred_element_type=F32
        )
        lanes = slice(16 * slot, 16 * slot + 16)
        for side in range(2):
            acc_ref[side * 3, :, lanes] = plain[:, 16 * side : 16 * side + 16]
            acc_ref[side * 3 + 1, :, lanes] = both[:, 32 * side : 32 * side + 16]
            acc_ref[side * 3 + 2, :, lanes] = both[:, 32 * side + 16 : 32 * side + 32]
    for side in range(2):
        for field in range(3):
            start = side * pairs * 12 + field * 4 + group
            out_ref[pl.ds(start, pairs, stride=12), :] = acc_ref[side * 3 + field]


def legendre_sums(legendre, harmonics, orders):
    slots, pairs, width = legendre.shape[1:]
    return pl.pallas_call(
        legendre_kernel,
        in_specs=[pl.BlockSpec(memory_space=pltpu.HBM)] * 3,
        out_specs=pl.BlockSpec(memory_space=pltpu.VMEM),
        scratch_shapes=[
            pltpu.SMEM(orders.shape, jnp.int32),
            pltpu.VMEM((3, slots, pairs, width), BF16),
            pltpu.VMEM(harmonics.shape, BF16),
            pltpu.VMEM((8, 96, 2 * width), BF16),
            pltpu.VMEM((6, pairs, 128), F32),
            pltpu.SemaphoreType.DMA((2, slots // 8)),
            pltpu.SemaphoreType.DMA,
        ],
        out_shape=jax.ShapeDtypeStruct((2 * pairs * 12, 128), F32),
        name="legendre_sums",
    )(orders, legendre, harmonics)


def cos_sin(phase):
    quarter = (phase + 2048) >> 12
    x = (phase - (quarter << 12)).astype(F32) * (math.pi / 8192)
    y = x * x
    sine = x + x * y * (-1.6666667e-1 + y * (8.3333310e-3 + y * (-1.9840874e-4 + y * 2.7525562e-6)))
    cosine = 1.0 + y * (-0.5 + y * (4.16666642e-2 + y * (-1.38887875e-3 + y * 2.4760495e-5)))
    swap = (quarter & 1) == 1
    cos_out = jnp.where(swap, sine, cosine)
    sin_out = jnp.where(swap, cosine, sine)
    cos_flip = ((quarter + 1) & 2) == 2
    sin_flip = (quarter & 2) == 2
    return jnp.where(cos_flip, -cos_out, cos_out), jnp.where(sin_flip, -sin_out, sin_out)


def high_low(value):
    high = value.astype(BF16)
    return high, (value - high.astype(F32)).astype(BF16)


def tables_kernel(cycle_ref, slots_ref, lower_ref, cos_ref, sin_ref, table_ref, table_buf, sem):
    slots = table_ref.shape[3]
    tiles = slots // 128
    shift = cycle_ref[lax.axis_index("ma") % cycle_ref.shape[0]] % 2
    row = lax.broadcasted_iota(jnp.int32, (16, 128), 0)
    turned = slots_ref[...].astype(F32).T
    pieces = []
    for middle in range(2):
        for device in range(4):
            start = device * 32 + middle * 8
            pieces.append(
                jnp.concatenate([turned[start : start + 8], turned[start + 16 : start + 24]], axis=0)
            )
    lower_ref[...] = jnp.concatenate(pieces, axis=1).astype(jnp.int32)

    def one_tile(tile):
        lower = lower_ref[pl.ds(tile, 1), :]
        odd = lower % 2
        lanes = pl.ds(pl.multiple_of(tile * 128, 128), 128)
        for parity in range(2):
            order = jnp.where(odd == parity, lower, 4095 - lower)
            factor = jnp.where(order == 0, 1.0, 2.0).astype(F32)
            cosine, sine = cos_sin((order * (512 * row + (255 + shift))) & 16383)
            cos_ref[parity, tile] = cosine * factor
            sin_ref[parity, tile] = sine * factor
            cos_v, sin_v = cos_sin((order * (2 * row + 1)) & 16383)
            cos_u, sin_u = cos_sin((order * (32 * row[0:8])) & 16383)
            for u in range(8):
                cu = cos_u[u : u + 1, :]
                su = sin_u[u : u + 1, :]
                for part, value in enumerate((cu * cos_v - su * sin_v, su * cos_v + cu * sin_v)):
                    high, low = high_low(value)
                    table_buf[parity, part, 16 * u : 16 * u + 16, lanes] = high
                    table_buf[parity, part, 128 + 16 * u : 144 + 16 * u, lanes] = low

    copies = []
    span = 4
    for block in range(tiles // span):
        pl.loop(block * span, (block + 1) * span)(one_tile)
        for parity in range(2):
            for part in range(2):
                view = (parity, part, slice(None), pl.ds(block * span * 128, span * 128))
                copy = pltpu.make_async_copy(table_buf.at[view], table_ref.at[view], sem.at[len(copies)])
                copy.start()
                copies.append(copy)
    for copy in copies:
        copy.wait()


def tables(cycle_index, slot_orders):
    slots = slot_orders.shape[0]
    vmem = pl.BlockSpec(memory_space=pltpu.VMEM)
    hbm = pl.BlockSpec(memory_space=pltpu.HBM)
    small = jax.ShapeDtypeStruct((2, slots // 128, 16, 128), F32)
    return pl.pallas_call(
        tables_kernel,
        in_specs=[pl.BlockSpec(memory_space=pltpu.SMEM), vmem],
        out_specs=[vmem, vmem, vmem, hbm],
        out_shape=[
            jax.ShapeDtypeStruct((slots // 128, 128), jnp.int32),
            small,
            small,
            jax.ShapeDtypeStruct((2, 2, 256, slots), BF16),
        ],
        scratch_shapes=[
            pltpu.VMEM((2, 2, 256, slots), BF16),
            pltpu.SemaphoreType.DMA((slots // 128,)),
        ],
        compiler_params=pltpu.CompilerParams(vmem_limit_bytes=52 << 20),
        name="tables",
    )(cycle_index, slot_orders.reshape(slots // 128, 128))


def synthesis_kernel(lower_ref, cos_ref, sin_ref, table_ref, sums_ref, out_ref, x_ref, a_ref, table_buf, sem):
    slots = table_ref.shape[3]
    tiles = slots // 128
    copies = [
        pltpu.make_async_copy(table_ref.at[parity], table_buf.at[parity], sem.at[parity]) for parity in range(2)
    ]
    for copy in copies:
        copy.start()
    for field in range(3):
        for pair in range(2):
            pieces = []
            for middle in range(2):
                for device in range(4):
                    start = device * 12 + field * 4 + pair * 2 + middle
                    pieces.append(sums_ref[pl.ds(start, 16, stride=48), :])
            turned = jnp.concatenate(pieces, axis=0).T
            turned = turned.reshape(8, 16, 128)
            odd = (lower_ref[pair * 8 : pair * 8 + 8, :] % 2 == 1)[:, None, :]
            x_ref[0, field, pair * 8 : pair * 8 + 8] = jnp.where(odd, turned[:, 8:16], turned[:, 0:8])
            x_ref[1, field, pair * 8 : pair * 8 + 8] = jnp.where(odd, turned[:, 0:8], turned[:, 8:16])

    @pl.loop(0, tiles)
    def _(tile):
        lanes = pl.ds(pl.multiple_of(tile * 128, 128), 128)

        @pl.loop(0, 2)
        def _(parity):
            cosine = cos_ref[parity, tile]
            sine = sin_ref[parity, tile]
            for field in range(3):
                for comp in range(4):
                    real = x_ref[parity, field, tile, pl.ds(comp, 16, stride=0), :]
                    imag = x_ref[parity, field, tile, pl.ds(4 + comp, 16, stride=0), :]
                    rows = (field * 4 + comp) * 16
                    for part, value in enumerate(
                        (real * cosine - imag * sine, -(real * sine + imag * cosine))
                    ):
                        high, low = high_low(value)
                        a_ref[parity, part, rows : rows + 16, lanes] = high
                        a_ref[parity, part, 192 + rows : 208 + rows, lanes] = low

    sides = []
    for parity in range(2):
        copies[parity].wait()
        both = []
        for part in range(2):
            wide = lax.dot_general(
                a_ref[parity, part], table_buf[parity, part], NT, preferred_element_type=F32
            )
            fine = wide[0:192, 128:256] + wide[192:384, 128:256]
            both.append(wide[0:192, 0:128] + (wide[192:384, 0:128] + fine))
        sides.append((both[0] - both[1], both[0] + both[1]))
    for side in range(2):
        lanes = slice(side * 128, side * 128 + 128)
        near = sides[0][side] + sides[1][side]
        far = sides[0][side] - sides[1][side]
        for block in range(4):
            for row in range(12):
                place = slice(row * 4, row * 4 + 4)
                source = slice(row * 16 + block * 4, row * 16 + block * 4 + 4)
                out_ref[block, place, lanes] = near[source, :]
                out_ref[block + 4, place, lanes] = far[source, :]


def synthesis(lower, cosine, sine, table, sums):
    vmem = pl.BlockSpec(memory_space=pltpu.VMEM)
    hbm = pl.BlockSpec(memory_space=pltpu.HBM)
    slots = table.shape[3]
    return pl.pallas_call(
        synthesis_kernel,
        in_specs=[vmem, vmem, vmem, hbm, vmem],
        out_specs=vmem,
        out_shape=jax.ShapeDtypeStruct((8, 48, 256), F32),
        scratch_shapes=[
            pltpu.VMEM((2, 3, slots // 128, 8, 128), F32),
            pltpu.VMEM((2, 2, 384, slots), BF16),
            pltpu.VMEM((2, 2, 256, slots), BF16),
            pltpu.SemaphoreType.DMA((2,)),
        ],
        compiler_params=pltpu.CompilerParams(vmem_limit_bytes=52 << 20),
        name="synthesis",
    )(lower, cosine, sine, table, sums)


def total_kernel(parts_ref, out_ref, sum_ref):
    total = parts_ref[0]
    for source in range(1, 8):
        total = total + parts_ref[source]
    falling = 127 - lax.broadcasted_iota(jnp.int32, (48, 128), 1)
    sum_ref[0] = jnp.take_along_axis(total[:, 0:128], falling, axis=1)
    sum_ref[1] = total[:, 128:256]
    for field in range(3):
        for piece in range(4):
            for side in range(2):
                start = piece * 256 + side * 128
                out_ref[0, field, :, start : start + 128] = sum_ref[side, pl.ds(field * 16 + piece, 4, stride=4), :]


def total(parts):
    vmem = pl.BlockSpec(memory_space=pltpu.VMEM)
    return pl.pallas_call(
        total_kernel,
        in_specs=[vmem],
        out_specs=vmem,
        out_shape=jax.ShapeDtypeStruct((1, 3, 4, 1024), F32),
        scratch_shapes=[pltpu.VMEM((2, 48, 128), F32)],
        compiler_params=pltpu.CompilerParams(vmem_limit_bytes=8 << 20),
        name="total",
    )(parts)


def body(legendre, harmonics, slot_orders, cycle_index):
    sums = legendre_sums(legendre, harmonics, slot_orders)
    moved = lax.all_to_all(sums.reshape(64, 3, 4, 128), "ma", split_axis=0, concat_axis=0, tiled=True)
    lower, cosine, sine, table = tables(cycle_index, slot_orders)
    blocks = synthesis(lower, cosine, sine, table, moved.reshape(768, 128))
    arrived = lax.all_to_all(blocks, "ell", split_axis=0, concat_axis=0, tiled=True)
    return total(arrived)


def solution(mesh):
    return jax.shard_map(
        body,
        mesh=mesh,
        in_specs=(P(None, "ma", None, "ell"), P("ma", None, None, None, "ell"), P(), P()),
        out_specs=P("ma", None, None, "ell"),
        check_vma=False,
    )
```

```python
import math

import jax
import jax.numpy as jnp
from jax import lax
from jax.experimental import pallas as pl
from jax.experimental.pallas import tpu as pltpu
from jax.sharding import PartitionSpec as P

F32 = jnp.float32
BF16 = jnp.bfloat16
NT = (((1,), (1,)), ((), ()))


def legendre_kernel(
    orders_hbm, leg_hbm, harm_hbm, out_ref, orders_ref, leg_all, harm_all, pack_ref, acc_ref, sem, orders_sem
):
    groups = leg_hbm.shape[1] // 8
    orders_copy = pltpu.make_async_copy(orders_hbm, orders_ref, orders_sem)
    orders_copy.start()

    def arrivals(group):
        span = pl.ds(group * 8, 8)
        return (
            pltpu.make_async_copy(harm_hbm.at[span], harm_all.at[span], sem.at[0, group]),
            pltpu.make_async_copy(leg_hbm.at[:, span], leg_all.at[:, span], sem.at[1, group]),
        )

    for group in range(groups):
        for copy in arrivals(group):
            copy.start()
    orders_copy.wait()

    @pl.loop(0, groups)
    def _(group):
        for copy in arrivals(group):
            copy.wait()
        span = pl.ds(group * 8, 8)
        legendre_group(
            group, groups, orders_ref, leg_all.at[:, span], harm_all.at[span], out_ref, pack_ref, acc_ref
        )


def legendre_group(group, groups, orders_ref, leg_ref, harm_ref, out_ref, pack_ref, acc_ref):
    pairs = leg_ref.shape[2]
    width = leg_ref.shape[3]
    full = 2 * orders_ref.shape[0]
    first_slot = lax.axis_index("ma") * (8 * groups) + group * 8
    column = lax.axis_index("ell") * width + lax.broadcasted_iota(jnp.int32, (1, width), 1)
    column_sign = (1 - 2 * (column % 2)).astype(F32)
    half = lax.broadcasted_iota(jnp.int32, (8, width), 0) < 4
    upper_rows = lax.broadcasted_iota(jnp.int32, (16, width), 0) >= 8
    for slot in range(8):
        lower = orders_ref[first_slot + slot]
        boundary = full - 1 - lower
        past = column >= boundary
        inside = (column < full - 1) & (past == upper_rows)
        weights = jnp.where(inside, 1.0, 0.0).astype(F32)
        flips = column_sign * jnp.where(upper_rows, (2 * (lower % 2) - 1).astype(F32), 1.0)
        signed = weights * flips
        temp, emode, bmode = (
            jnp.concatenate([harm_ref[slot, kind, part].astype(F32) for part in range(2)], axis=0)
            for kind in range(3)
        )
        eturn = pltpu.roll(emode, 4, 0)
        eturn = jnp.where(half, -eturn, eturn)
        bturn = pltpu.roll(bmode, 4, 0)
        bturn = jnp.where(half, bturn, -bturn)

        def twice(values):
            return jnp.concatenate([values, values], axis=0).astype(BF16)

        temp, emode, bmode = twice(temp), twice(-emode), twice(-bmode)
        eturn, bturn = twice(eturn), twice(bturn)
        for side in range(2):
            straight = (signed if side else weights).astype(BF16)
            turned = (-signed).astype(BF16) if side else straight
            base = side * 32
            pack_ref[slot, base : base + 16, 0:width] = emode * straight
            pack_ref[slot, base : base + 16, width : 2 * width] = bturn * turned
            pack_ref[slot, base + 16 : base + 32, 0:width] = bmode * straight
            pack_ref[slot, base + 16 : base + 32, width : 2 * width] = eturn * turned
            pack_ref[slot, 64 + side * 16 : 80 + side * 16, 0:width] = temp * straight
        both = lax.dot_general(
            jnp.concatenate([leg_ref[1, slot], leg_ref[2, slot]], axis=1),
            pack_ref[slot, 0:64],
            NT,
            preferred_element_type=F32,
        )
        plain = lax.dot_general(
            leg_ref[0, slot], pack_ref[slot, 64:96, 0:width], NT, preferred_element_type=F32
        )
        lanes = slice(16 * slot, 16 * slot + 16)
        for side in range(2):
            acc_ref[side * 3, :, lanes] = plain[:, 16 * side : 16 * side + 16]
            acc_ref[side * 3 + 1, :, lanes] = both[:, 32 * side : 32 * side + 16]
            acc_ref[side * 3 + 2, :, lanes] = both[:, 32 * side + 16 : 32 * side + 32]
    for side in range(2):
        for field in range(3):
            start = side * pairs * 12 + field * 4 + group
            out_ref[pl.ds(start, pairs, stride=12), :] = acc_ref[side * 3 + field]


def legendre_sums(legendre, harmonics, orders):
    slots, pairs, width = legendre.shape[1:]
    return pl.pallas_call(
        legendre_kernel,
        in_specs=[pl.BlockSpec(memory_space=pltpu.HBM)] * 3,
        out_specs=pl.BlockSpec(memory_space=pltpu.VMEM),
        scratch_shapes=[
            pltpu.SMEM(orders.shape, jnp.int32),
            pltpu.VMEM((3, slots, pairs, width), BF16),
            pltpu.VMEM(harmonics.shape, BF16),
            pltpu.VMEM((8, 96, 2 * width), BF16),
            pltpu.VMEM((6, pairs, 128), F32),
            pltpu.SemaphoreType.DMA((2, slots // 8)),
            pltpu.SemaphoreType.DMA,
        ],
        out_shape=jax.ShapeDtypeStruct((2 * pairs * 12, 128), F32),
        name="legendre_sums",
    )(orders, legendre, harmonics)


def cos_sin(phase):
    quarter = (phase + 2048) >> 12
    x = (phase - (quarter << 12)).astype(F32) * (math.pi / 8192)
    y = x * x
    sine = x + x * y * (-1.6666667e-1 + y * (8.3333310e-3 + y * (-1.9840874e-4 + y * 2.7525562e-6)))
    cosine = 1.0 + y * (-0.5 + y * (4.16666642e-2 + y * (-1.38887875e-3 + y * 2.4760495e-5)))
    swap = (quarter & 1) == 1
    cos_out = jnp.where(swap, sine, cosine)
    sin_out = jnp.where(swap, cosine, sine)
    cos_flip = ((quarter + 1) & 2) == 2
    sin_flip = (quarter & 2) == 2
    return jnp.where(cos_flip, -cos_out, cos_out), jnp.where(sin_flip, -sin_out, sin_out)


def high_low(value):
    high = value.astype(BF16)
    return high, (value - high.astype(F32)).astype(BF16)


def tables_kernel(cycle_ref, slots_ref, lower_ref, cos_ref, sin_ref, table_ref, table_buf, sem):
    slots = table_ref.shape[3]
    tiles = slots // 128
    shift = cycle_ref[lax.axis_index("ma") % cycle_ref.shape[0]] % 2
    row = lax.broadcasted_iota(jnp.int32, (16, 128), 0)
    turned = slots_ref[...].astype(F32).T
    pieces = []
    for middle in range(2):
        for device in range(4):
            start = device * 32 + middle * 8
            pieces.append(
                jnp.concatenate([turned[start : start + 8], turned[start + 16 : start + 24]], axis=0)
            )
    lower_ref[...] = jnp.concatenate(pieces, axis=1).astype(jnp.int32)

    def one_tile(tile):
        lower = lower_ref[pl.ds(tile, 1), :]
        odd = lower % 2
        lanes = pl.ds(pl.multiple_of(tile * 128, 128), 128)
        for parity in range(2):
            order = jnp.where(odd == parity, lower, 4095 - lower)
            factor = jnp.where(order == 0, 1.0, 2.0).astype(F32)
            cosine, sine = cos_sin((order * (512 * row + (255 + shift))) & 16383)
            cos_ref[parity, tile] = cosine * factor
            sin_ref[parity, tile] = -sine * factor
            cos_v, sin_v = cos_sin((order * (2 * row + 1)) & 16383)
            cos_u, sin_u = cos_sin((order * (32 * row[0:8])) & 16383)
            for u in range(8):
                cu = cos_u[u : u + 1, :]
                su = sin_u[u : u + 1, :]
                for part, value in enumerate((cu * cos_v - su * sin_v, su * cos_v + cu * sin_v)):
                    high, low = high_low(value)
                    table_buf[parity, part, 16 * u : 16 * u + 16, lanes] = high
                    table_buf[parity, part, 128 + 16 * u : 144 + 16 * u, lanes] = low

    copies = []
    span = 4
    for block in range(tiles // span):
        pl.loop(block * span, (block + 1) * span)(one_tile)
        for parity in range(2):
            for part in range(2):
                view = (parity, part, slice(None), pl.ds(block * span * 128, span * 128))
                copy = pltpu.make_async_copy(table_buf.at[view], table_ref.at[view], sem.at[len(copies)])
                copy.start()
                copies.append(copy)
    for copy in copies:
        copy.wait()


def tables(cycle_index, slot_orders):
    slots = slot_orders.shape[0]
    vmem = pl.BlockSpec(memory_space=pltpu.VMEM)
    hbm = pl.BlockSpec(memory_space=pltpu.HBM)
    small = jax.ShapeDtypeStruct((2, slots // 128, 16, 128), F32)
    return pl.pallas_call(
        tables_kernel,
        in_specs=[pl.BlockSpec(memory_space=pltpu.SMEM), vmem],
        out_specs=[vmem, vmem, vmem, hbm],
        out_shape=[
            jax.ShapeDtypeStruct((slots // 128, 128), jnp.int32),
            small,
            small,
            jax.ShapeDtypeStruct((2, 2, 256, slots), BF16),
        ],
        scratch_shapes=[
            pltpu.VMEM((2, 2, 256, slots), BF16),
            pltpu.SemaphoreType.DMA((slots // 128,)),
        ],
        compiler_params=pltpu.CompilerParams(vmem_limit_bytes=52 << 20),
        name="tables",
    )(cycle_index, slot_orders.reshape(slots // 128, 128))


def synthesis_kernel(lower_ref, cos_ref, sin_ref, table_ref, sums_ref, out_ref, x_ref, a_ref, table_buf, sem):
    slots = table_ref.shape[3]
    tiles = slots // 128
    copies = [
        pltpu.make_async_copy(
            table_ref.at[parity], table_buf.at[parity, :, :, pl.ds(0, slots)], sem.at[parity]
        )
        for parity in range(2)
    ]
    for copy in copies:
        copy.start()
    for field in range(3):
        for pair in range(2):
            pieces = []
            for middle in range(2):
                for device in range(4):
                    start = device * 12 + field * 4 + pair * 2 + middle
                    pieces.append(sums_ref[pl.ds(start, 16, stride=48), :])
            turned = jnp.concatenate(pieces, axis=0).T
            turned = turned.reshape(8, 16, 128)
            odd = (lower_ref[pair * 8 : pair * 8 + 8, :] % 2 == 1)[:, None, :]
            x_ref[0, field, pair * 8 : pair * 8 + 8] = jnp.where(odd, turned[:, 8:16], turned[:, 0:8])
            x_ref[1, field, pair * 8 : pair * 8 + 8] = jnp.where(odd, turned[:, 0:8], turned[:, 8:16])

    @pl.loop(0, tiles)
    def _(tile):
        lanes = pl.ds(pl.multiple_of(tile * 128, 128), 128)

        @pl.loop(0, 2, unroll=2)
        def _(parity):
            cosine = cos_ref[parity, tile]
            minus = sin_ref[parity, tile]
            for field in range(3):
                x = x_ref[parity, field, tile]
                for comp in range(4):
                    real = x[comp : comp + 1, :]
                    imag = x[4 + comp : 5 + comp, :]
                    rows = (field * 4 + comp) * 16
                    for part, value in enumerate((real * cosine + imag * minus, real * minus - imag * cosine)):
                        high, low = high_low(value)
                        a_ref[parity, part, rows : rows + 16, lanes] = high
                        a_ref[parity, part, 192 + rows : 208 + rows, lanes] = low

    sides = []
    for parity in range(2):
        copies[parity].wait()
        both = []
        for part in range(2):
            wide = lax.dot_general(
                a_ref[parity, part, :, 0:slots], table_buf[parity, part, :, 0:slots], NT, preferred_element_type=F32
            )
            fine = wide[0:192, 128:256] + wide[192:384, 128:256]
            both.append(wide[0:192, 0:128] + (wide[192:384, 0:128] + fine))
        sides.append((both[0] - both[1], both[0] + both[1]))
    for side in range(2):
        lanes = slice(side * 128, side * 128 + 128)
        near = sides[0][side] + sides[1][side]
        far = sides[0][side] - sides[1][side]
        for block in range(4):
            for row in range(12):
                place = slice(row * 4, row * 4 + 4)
                source = slice(row * 16 + block * 4, row * 16 + block * 4 + 4)
                out_ref[block, place, lanes] = near[source, :]
                out_ref[block + 4, place, lanes] = far[source, :]


def synthesis(lower, cosine, sine, table, sums):
    vmem = pl.BlockSpec(memory_space=pltpu.VMEM)
    hbm = pl.BlockSpec(memory_space=pltpu.HBM)
    slots = table.shape[3]
    return pl.pallas_call(
        synthesis_kernel,
        in_specs=[vmem, vmem, vmem, hbm, vmem],
        out_specs=vmem,
        out_shape=jax.ShapeDtypeStruct((8, 48, 256), F32),
        scratch_shapes=[
            pltpu.VMEM((2, 3, slots // 128, 8, 128), F32),
            pltpu.VMEM((2, 2, 384, slots + 128), BF16),
            pltpu.VMEM((2, 2, 256, slots + 128), BF16),
            pltpu.SemaphoreType.DMA((2,)),
        ],
        compiler_params=pltpu.CompilerParams(vmem_limit_bytes=52 << 20),
        name="synthesis",
    )(lower, cosine, sine, table, sums)


def total_kernel(parts_ref, out_ref, sum_ref):
    total = parts_ref[0]
    for source in range(1, 8):
        total = total + parts_ref[source]
    falling = 127 - lax.broadcasted_iota(jnp.int32, (48, 128), 1)
    sum_ref[0] = jnp.take_along_axis(total[:, 0:128], falling, axis=1)
    sum_ref[1] = total[:, 128:256]
    for field in range(3):
        for piece in range(4):
            for side in range(2):
                start = piece * 256 + side * 128
                out_ref[0, field, :, start : start + 128] = sum_ref[side, pl.ds(field * 16 + piece, 4, stride=4), :]


def total(parts):
    vmem = pl.BlockSpec(memory_space=pltpu.VMEM)
    return pl.pallas_call(
        total_kernel,
        in_specs=[vmem],
        out_specs=vmem,
        out_shape=jax.ShapeDtypeStruct((1, 3, 4, 1024), F32),
        scratch_shapes=[pltpu.VMEM((2, 48, 128), F32)],
        compiler_params=pltpu.CompilerParams(vmem_limit_bytes=8 << 20),
        name="total",
    )(parts)


def body(legendre, harmonics, slot_orders, cycle_index):
    sums = legendre_sums(legendre, harmonics, slot_orders)
    moved = lax.all_to_all(sums.reshape(64, 3, 4, 128), "ma", split_axis=0, concat_axis=0, tiled=True)
    lower, cosine, sine, table = tables(cycle_index, slot_orders)
    blocks = synthesis(lower, cosine, sine, table, moved.reshape(768, 128))
    arrived = lax.all_to_all(blocks, "ell", split_axis=0, concat_axis=0, tiled=True)
    return total(arrived)


def solution(mesh):
    return jax.shard_map(
        body,
        mesh=mesh,
        in_specs=(P(None, "ma", None, "ell"), P("ma", None, None, None, "ell"), P(), P()),
        out_specs=P("ma", None, None, "ell"),
        check_vma=False,
    )
```

```python
import math

import jax
import jax.numpy as jnp
from jax import lax
from jax.experimental import pallas as pl
from jax.experimental.pallas import tpu as pltpu
from jax.sharding import PartitionSpec as P

F32 = jnp.float32
BF16 = jnp.bfloat16
NT = (((1,), (1,)), ((), ()))


def legendre_kernel(
    orders_hbm, leg_hbm, harm_hbm, out_ref, orders_ref, leg_all, harm_all, pack_ref, acc_ref, sem, orders_sem
):
    groups = leg_hbm.shape[1] // 8
    orders_copy = pltpu.make_async_copy(orders_hbm, orders_ref, orders_sem)
    orders_copy.start()

    def arrivals(group):
        span = pl.ds(group * 8, 8)
        return (
            pltpu.make_async_copy(harm_hbm.at[span], harm_all.at[span], sem.at[0, group]),
            pltpu.make_async_copy(leg_hbm.at[:, span], leg_all.at[:, span], sem.at[1, group]),
        )

    for group in range(groups):
        for copy in arrivals(group):
            copy.start()
    orders_copy.wait()

    @pl.loop(0, groups)
    def _(group):
        for copy in arrivals(group):
            copy.wait()
        span = pl.ds(group * 8, 8)
        legendre_group(
            group, groups, orders_ref, leg_all.at[:, span], harm_all.at[span], out_ref, pack_ref, acc_ref
        )


def legendre_group(group, groups, orders_ref, leg_ref, harm_ref, out_ref, pack_ref, acc_ref):
    pairs = leg_ref.shape[2]
    width = leg_ref.shape[3]
    full = 2 * orders_ref.shape[0]
    first_slot = lax.axis_index("ma") * (8 * groups) + group * 8
    column = lax.axis_index("ell") * width + lax.broadcasted_iota(jnp.int32, (1, width), 1)
    column_sign = (1 - 2 * (column % 2)).astype(F32)
    half = lax.broadcasted_iota(jnp.int32, (8, width), 0) < 4
    upper_rows = lax.broadcasted_iota(jnp.int32, (16, width), 0) >= 8
    for slot in range(8):
        lower = orders_ref[first_slot + slot]
        boundary = full - 1 - lower
        past = column >= boundary
        inside = (column < full - 1) & (past == upper_rows)
        weights = jnp.where(inside, 1.0, 0.0).astype(F32)
        flips = column_sign * jnp.where(upper_rows, (2 * (lower % 2) - 1).astype(F32), 1.0)
        signed = weights * flips
        temp, emode, bmode = (
            jnp.concatenate([harm_ref[slot, kind, part].astype(F32) for part in range(2)], axis=0)
            for kind in range(3)
        )
        eturn = pltpu.roll(emode, 4, 0)
        eturn = jnp.where(half, -eturn, eturn)
        bturn = pltpu.roll(bmode, 4, 0)
        bturn = jnp.where(half, bturn, -bturn)

        def twice(values):
            return jnp.concatenate([values, values], axis=0).astype(BF16)

        temp, emode, bmode = twice(temp), twice(-emode), twice(-bmode)
        eturn, bturn = twice(eturn), twice(bturn)
        for side in range(2):
            straight = (signed if side else weights).astype(BF16)
            turned = (-signed).astype(BF16) if side else straight
            base = side * 32
            pack_ref[slot, base : base + 16, 0:width] = emode * straight
            pack_ref[slot, base : base + 16, width : 2 * width] = bturn * turned
            pack_ref[slot, base + 16 : base + 32, 0:width] = bmode * straight
            pack_ref[slot, base + 16 : base + 32, width : 2 * width] = eturn * turned
            pack_ref[slot, 64 + side * 16 : 80 + side * 16, 0:width] = temp * straight
        both = lax.dot_general(
            jnp.concatenate([leg_ref[1, slot], leg_ref[2, slot]], axis=1),
            pack_ref[slot, 0:64],
            NT,
            preferred_element_type=F32,
        )
        plain = lax.dot_general(
            leg_ref[0, slot], pack_ref[slot, 64:96, 0:width], NT, preferred_element_type=F32
        )
        lanes = slice(16 * slot, 16 * slot + 16)
        for side in range(2):
            acc_ref[side * 3, :, lanes] = plain[:, 16 * side : 16 * side + 16]
            acc_ref[side * 3 + 1, :, lanes] = both[:, 32 * side : 32 * side + 16]
            acc_ref[side * 3 + 2, :, lanes] = both[:, 32 * side + 16 : 32 * side + 32]
    for side in range(2):
        for field in range(3):
            start = (1 - side) * pairs * 12 + field * 4 + group
            out_ref[pl.ds(start, pairs, stride=12), :] = acc_ref[side * 3 + field]


def legendre_sums(legendre, harmonics, orders):
    slots, pairs, width = legendre.shape[1:]
    return pl.pallas_call(
        legendre_kernel,
        in_specs=[pl.BlockSpec(memory_space=pltpu.HBM)] * 3,
        out_specs=pl.BlockSpec(memory_space=pltpu.VMEM),
        scratch_shapes=[
            pltpu.SMEM(orders.shape, jnp.int32),
            pltpu.VMEM((3, slots, pairs, width), BF16),
            pltpu.VMEM(harmonics.shape, BF16),
            pltpu.VMEM((8, 96, 2 * width), BF16),
            pltpu.VMEM((6, pairs, 128), F32),
            pltpu.SemaphoreType.DMA((2, slots // 8)),
            pltpu.SemaphoreType.DMA,
        ],
        out_shape=jax.ShapeDtypeStruct((2 * pairs * 12, 128), F32),
        name="legendre_sums",
    )(orders, legendre, harmonics)


def cos_sin(phase):
    quarter = (phase + 2048) >> 12
    x = (phase - (quarter << 12)).astype(F32) * (math.pi / 8192)
    y = x * x
    sine = x + x * y * (-1.6666667e-1 + y * (8.3333310e-3 + y * (-1.9840874e-4 + y * 2.7525562e-6)))
    cosine = 1.0 + y * (-0.5 + y * (4.16666642e-2 + y * (-1.38887875e-3 + y * 2.4760495e-5)))
    swap = (quarter & 1) == 1
    cos_out = jnp.where(swap, sine, cosine)
    sin_out = jnp.where(swap, cosine, sine)
    cos_flip = ((quarter + 1) & 2) == 2
    sin_flip = (quarter & 2) == 2
    return jnp.where(cos_flip, -cos_out, cos_out), jnp.where(sin_flip, -sin_out, sin_out)


def high_low(value):
    high = value.astype(BF16)
    return high, (value - high.astype(F32)).astype(BF16)


def tables_kernel(cycle_ref, slots_ref, lower_ref, cos_ref, sin_ref, table_ref, table_buf, sem):
    slots = table_ref.shape[3]
    tiles = slots // 128
    shift = cycle_ref[lax.axis_index("ma") % cycle_ref.shape[0]] % 2
    row = lax.broadcasted_iota(jnp.int32, (16, 128), 0)
    turned = jnp.concatenate([slots_ref[8:16, :], slots_ref[0:8, :]], axis=0).astype(F32).T
    pieces = []
    for middle in range(2):
        for device in range(4):
            start = device * 32 + middle * 8
            pieces.append(
                jnp.concatenate([turned[start : start + 8], turned[start + 16 : start + 24]], axis=0)
            )
    lower_ref[...] = jnp.concatenate(pieces, axis=1).astype(jnp.int32)

    def one_tile(tile):
        lower = lower_ref[pl.ds(tile, 1), :]
        odd = lower % 2
        lanes = pl.ds(pl.multiple_of(tile * 128, 128), 128)
        for parity in range(2):
            order = jnp.where(odd == parity, lower, 4095 - lower)
            factor = jnp.where(order == 0, 1.0, 2.0).astype(F32)
            cosine, sine = cos_sin((order * (512 * row + (255 + shift))) & 16383)
            cos_ref[parity, tile] = cosine * factor
            sin_ref[parity, tile] = -sine * factor
            cos_v, sin_v = cos_sin((order * (2 * row + 1)) & 16383)
            cos_u, sin_u = cos_sin((order * (32 * row[0:8])) & 16383)
            for u in range(8):
                cu = cos_u[u : u + 1, :]
                su = sin_u[u : u + 1, :]
                for part, value in enumerate((cu * cos_v - su * sin_v, su * cos_v + cu * sin_v)):
                    high, low = high_low(value)
                    table_buf[parity, part, 16 * u : 16 * u + 16, lanes] = high
                    table_buf[parity, part, 128 + 16 * u : 144 + 16 * u, lanes] = low

    copies = []
    span = 4
    for block in range(tiles // span):
        pl.loop(block * span, (block + 1) * span)(one_tile)
        for parity in range(2):
            for part in range(2):
                view = (parity, part, slice(None), pl.ds(block * span * 128, span * 128))
                copy = pltpu.make_async_copy(table_buf.at[view], table_ref.at[view], sem.at[len(copies)])
                copy.start()
                copies.append(copy)
    for copy in copies:
        copy.wait()


def tables(cycle_index, slot_orders):
    slots = slot_orders.shape[0]
    vmem = pl.BlockSpec(memory_space=pltpu.VMEM)
    hbm = pl.BlockSpec(memory_space=pltpu.HBM)
    small = jax.ShapeDtypeStruct((2, slots // 128, 16, 128), F32)
    return pl.pallas_call(
        tables_kernel,
        in_specs=[pl.BlockSpec(memory_space=pltpu.SMEM), vmem],
        out_specs=[vmem, vmem, vmem, hbm],
        out_shape=[
            jax.ShapeDtypeStruct((slots // 128, 128), jnp.int32),
            small,
            small,
            jax.ShapeDtypeStruct((2, 2, 256, slots), BF16),
        ],
        scratch_shapes=[
            pltpu.VMEM((2, 2, 256, slots), BF16),
            pltpu.SemaphoreType.DMA((slots // 128,)),
        ],
        compiler_params=pltpu.CompilerParams(vmem_limit_bytes=52 << 20),
        name="tables",
    )(cycle_index, slot_orders.reshape(slots // 128, 128))


def synthesis_kernel(lower_ref, cos_ref, sin_ref, table_ref, sums_ref, out_ref, x_ref, a_ref, table_buf, sem):
    slots = table_ref.shape[3]
    tiles = slots // 128
    copies = [
        pltpu.make_async_copy(
            table_ref.at[parity], table_buf.at[parity, :, :, pl.ds(0, slots)], sem.at[parity]
        )
        for parity in range(2)
    ]
    for copy in copies:
        copy.start()
    for field in range(3):
        for pair in range(2):
            pieces = []
            for middle in range(2):
                for device in range(4):
                    start = device * 12 + field * 4 + pair * 2 + middle
                    pieces.append(sums_ref[pl.ds(start, 16, stride=48), :])
            turned = jnp.concatenate(pieces, axis=0).T
            turned = turned.reshape(8, 16, 128)
            odd = (lower_ref[pair * 8 : pair * 8 + 8, :] % 2 == 1)[:, None, :]
            x_ref[0, field, pair * 8 : pair * 8 + 8] = jnp.where(odd, turned[:, 8:16], turned[:, 0:8])
            x_ref[1, field, pair * 8 : pair * 8 + 8] = jnp.where(odd, turned[:, 0:8], turned[:, 8:16])

    @pl.loop(0, tiles)
    def _(tile):
        lanes = pl.ds(pl.multiple_of(tile * 128, 128), 128)

        @pl.loop(0, 2, unroll=2)
        def _(parity):
            cosine = cos_ref[parity, tile]
            minus = sin_ref[parity, tile]
            for field in range(3):
                x = x_ref[parity, field, tile]
                for comp in range(4):
                    real = x[comp : comp + 1, :]
                    imag = x[4 + comp : 5 + comp, :]
                    rows = (field * 4 + comp) * 16
                    for part, value in enumerate((real * cosine + imag * minus, real * minus - imag * cosine)):
                        high, low = high_low(value)
                        a_ref[parity, part, rows : rows + 16, lanes] = high
                        a_ref[parity, part, 192 + rows : 208 + rows, lanes] = low

    sides = []
    for parity in range(2):
        copies[parity].wait()
        both = []
        for part in range(2):
            wide = lax.dot_general(
                a_ref[parity, part, :, 0:slots], table_buf[parity, part, :, 0:slots], NT, preferred_element_type=F32
            )
            fine = wide[0:192, 128:256] + wide[192:384, 128:256]
            both.append(wide[0:192, 0:128] + (wide[192:384, 0:128] + fine))
        sides.append((both[0] - both[1], both[0] + both[1]))
    for side in range(2):
        lanes = slice(side * 128, side * 128 + 128)
        near = sides[0][side] + sides[1][side]
        far = sides[0][side] - sides[1][side]
        for block in range(4):
            for row in range(12):
                place = slice(row * 4, row * 4 + 4)
                source = slice(row * 16 + block * 4, row * 16 + block * 4 + 4)
                out_ref[block, place, lanes] = near[source, :]
                out_ref[block + 4, place, lanes] = far[source, :]


def synthesis(lower, cosine, sine, table, sums):
    vmem = pl.BlockSpec(memory_space=pltpu.VMEM)
    hbm = pl.BlockSpec(memory_space=pltpu.HBM)
    slots = table.shape[3]
    return pl.pallas_call(
        synthesis_kernel,
        in_specs=[vmem, vmem, vmem, hbm, vmem],
        out_specs=vmem,
        out_shape=jax.ShapeDtypeStruct((8, 48, 256), F32),
        scratch_shapes=[
            pltpu.VMEM((2, 3, slots // 128, 8, 128), F32),
            pltpu.VMEM((2, 2, 384, slots + 128), BF16),
            pltpu.VMEM((2, 2, 256, slots + 128), BF16),
            pltpu.SemaphoreType.DMA((2,)),
        ],
        compiler_params=pltpu.CompilerParams(vmem_limit_bytes=52 << 20),
        name="synthesis",
    )(lower, cosine, sine, table, sums)


def total_kernel(parts_ref, out_ref, sum_ref):
    total = parts_ref[0]
    for source in range(1, 8):
        total = total + parts_ref[source]
    falling = 127 - lax.broadcasted_iota(jnp.int32, (48, 128), 1)
    sum_ref[0] = jnp.take_along_axis(total[:, 0:128], falling, axis=1)
    sum_ref[1] = total[:, 128:256]
    for field in range(3):
        for piece in range(4):
            for side in range(2):
                start = piece * 256 + side * 128
                out_ref[0, field, :, start : start + 128] = sum_ref[side, pl.ds(field * 16 + piece, 4, stride=4), :]


def total(parts):
    vmem = pl.BlockSpec(memory_space=pltpu.VMEM)
    return pl.pallas_call(
        total_kernel,
        in_specs=[vmem],
        out_specs=vmem,
        out_shape=jax.ShapeDtypeStruct((1, 3, 4, 1024), F32),
        scratch_shapes=[pltpu.VMEM((2, 48, 128), F32)],
        compiler_params=pltpu.CompilerParams(vmem_limit_bytes=8 << 20),
        name="total",
    )(parts)


def body(legendre, harmonics, slot_orders, cycle_index):
    sums = legendre_sums(legendre, harmonics, slot_orders)
    swapped = [[device ^ 32 for device in range(64)]]
    moved = lax.all_to_all(
        sums.reshape(64, 3, 4, 128), "ma", split_axis=0, concat_axis=0, axis_index_groups=swapped, tiled=True
    )
    lower, cosine, sine, table = tables(cycle_index, slot_orders)
    blocks = synthesis(lower, cosine, sine, table, moved.reshape(768, 128))
    arrived = lax.all_to_all(blocks, "ell", split_axis=0, concat_axis=0, tiled=True)
    return total(arrived)


def solution(mesh):
    return jax.shard_map(
        body,
        mesh=mesh,
        in_specs=(P(None, "ma", None, "ell"), P("ma", None, None, None, "ell"), P(), P()),
        out_specs=P("ma", None, None, "ell"),
        check_vma=False,
    )
```

```python
import math

import jax
import jax.numpy as jnp
from jax import lax
from jax.experimental import pallas as pl
from jax.experimental.pallas import tpu as pltpu
from jax.sharding import PartitionSpec as P

F32 = jnp.float32
BF16 = jnp.bfloat16
NT = (((1,), (1,)), ((), ()))


def legendre_kernel(
    orders_hbm, leg_hbm, harm_hbm, out_ref, orders_ref, leg_all, harm_all, pack_ref, acc_ref, sem, orders_sem
):
    groups = leg_hbm.shape[1] // 8
    orders_copy = pltpu.make_async_copy(orders_hbm, orders_ref, orders_sem)
    orders_copy.start()

    def arrivals(group):
        span = pl.ds(group * 8, 8)
        return (
            pltpu.make_async_copy(harm_hbm.at[span], harm_all.at[span], sem.at[0, group]),
            pltpu.make_async_copy(leg_hbm.at[:, span], leg_all.at[:, span], sem.at[1, group]),
        )

    for group in range(groups):
        for copy in arrivals(group):
            copy.start()
    orders_copy.wait()

    @pl.loop(0, groups)
    def _(group):
        for copy in arrivals(group):
            copy.wait()
        span = pl.ds(group * 8, 8)
        legendre_group(
            group, groups, orders_ref, leg_all.at[:, span], harm_all.at[span], out_ref, pack_ref, acc_ref
        )


def legendre_group(group, groups, orders_ref, leg_ref, harm_ref, out_ref, pack_ref, acc_ref):
    pairs = leg_ref.shape[2]
    width = leg_ref.shape[3]
    full = 2 * orders_ref.shape[0]
    first_slot = lax.axis_index("ma") * (8 * groups) + group * 8
    column = lax.axis_index("ell") * width + lax.broadcasted_iota(jnp.int32, (1, width), 1)
    column_sign = (1 - 2 * (column % 2)).astype(F32)
    half = lax.broadcasted_iota(jnp.int32, (8, width), 0) < 4
    upper_rows = lax.broadcasted_iota(jnp.int32, (16, width), 0) >= 8
    for slot in range(8):
        lower = orders_ref[first_slot + slot]
        boundary = full - 1 - lower
        past = column >= boundary
        inside = (column < full - 1) & (past == upper_rows)
        weights = jnp.where(inside, 1.0, 0.0).astype(F32)
        flips = column_sign * jnp.where(upper_rows, (2 * (lower % 2) - 1).astype(F32), 1.0)
        signed = weights * flips
        temp, emode, bmode = (
            jnp.concatenate([harm_ref[slot, kind, part].astype(F32) for part in range(2)], axis=0)
            for kind in range(3)
        )
        eturn = pltpu.roll(emode, 4, 0)
        eturn = jnp.where(half, -eturn, eturn)
        bturn = pltpu.roll(bmode, 4, 0)
        bturn = jnp.where(half, bturn, -bturn)

        def twice(values):
            return jnp.concatenate([values, values], axis=0).astype(BF16)

        temp, emode, bmode = twice(temp), twice(-emode), twice(-bmode)
        eturn, bturn = twice(eturn), twice(bturn)
        for side in range(2):
            straight = (signed if side else weights).astype(BF16)
            turned = (-signed).astype(BF16) if side else straight
            base = side * 32
            pack_ref[slot, base : base + 16, 0:width] = emode * straight
            pack_ref[slot, base : base + 16, width : 2 * width] = bturn * turned
            pack_ref[slot, base + 16 : base + 32, 0:width] = bmode * straight
            pack_ref[slot, base + 16 : base + 32, width : 2 * width] = eturn * turned
            pack_ref[slot, 64 + side * 16 : 80 + side * 16, 0:width] = temp * straight
        both = lax.dot_general(
            jnp.concatenate([leg_ref[1, slot], leg_ref[2, slot]], axis=1),
            pack_ref[slot, 0:64],
            NT,
            preferred_element_type=F32,
        )
        plain = lax.dot_general(
            leg_ref[0, slot], pack_ref[slot, 64:96, 0:width], NT, preferred_element_type=F32
        )
        lanes = slice(16 * slot, 16 * slot + 16)
        for side in range(2):
            acc_ref[side * 3, :, lanes] = plain[:, 16 * side : 16 * side + 16]
            acc_ref[side * 3 + 1, :, lanes] = both[:, 32 * side : 32 * side + 16]
            acc_ref[side * 3 + 2, :, lanes] = both[:, 32 * side + 16 : 32 * side + 32]
    for side in range(2):
        for field in range(3):
            start = (1 - side) * pairs * 12 + field * 4 + group
            out_ref[pl.ds(start, pairs, stride=12), :] = acc_ref[side * 3 + field]


def legendre_sums(legendre, harmonics, orders):
    slots, pairs, width = legendre.shape[1:]
    return pl.pallas_call(
        legendre_kernel,
        in_specs=[pl.BlockSpec(memory_space=pltpu.HBM)] * 3,
        out_specs=pl.BlockSpec(memory_space=pltpu.VMEM),
        scratch_shapes=[
            pltpu.SMEM(orders.shape, jnp.int32),
            pltpu.VMEM((3, slots, pairs, width), BF16),
            pltpu.VMEM(harmonics.shape, BF16),
            pltpu.VMEM((8, 96, 2 * width), BF16),
            pltpu.VMEM((6, pairs, 128), F32),
            pltpu.SemaphoreType.DMA((2, slots // 8)),
            pltpu.SemaphoreType.DMA,
        ],
        out_shape=jax.ShapeDtypeStruct((2 * pairs * 12, 128), F32),
        name="legendre_sums",
    )(orders, legendre, harmonics)


def cos_sin(phase):
    quarter = (phase + 2048) >> 12
    x = (phase - (quarter << 12)).astype(F32) * (math.pi / 8192)
    y = x * x
    sine = x + x * y * (-1.6666667e-1 + y * (8.3333310e-3 + y * (-1.9840874e-4 + y * 2.7525562e-6)))
    cosine = 1.0 + y * (-0.5 + y * (4.16666642e-2 + y * (-1.38887875e-3 + y * 2.4760495e-5)))
    swap = (quarter & 1) == 1
    cos_out = jnp.where(swap, sine, cosine)
    sin_out = jnp.where(swap, cosine, sine)
    cos_flip = ((quarter + 1) & 2) == 2
    sin_flip = (quarter & 2) == 2
    return jnp.where(cos_flip, -cos_out, cos_out), jnp.where(sin_flip, -sin_out, sin_out)


def high_low(value):
    high = value.astype(BF16)
    return high, (value - high.astype(F32)).astype(BF16)


def tables_kernel(cycle_ref, slots_ref, lower_ref, cos_ref, sin_ref, table_ref, table_buf, sem):
    slots = table_ref.shape[3]
    tiles = slots // 128
    shift = cycle_ref[lax.axis_index("ma") % cycle_ref.shape[0]] % 2
    row = lax.broadcasted_iota(jnp.int32, (16, 128), 0)
    turned = jnp.concatenate([slots_ref[8:16, :], slots_ref[0:8, :]], axis=0).astype(F32).T
    pieces = []
    for middle in range(2):
        for device in range(4):
            start = device * 32 + middle * 8
            pieces.append(
                jnp.concatenate([turned[start : start + 8], turned[start + 16 : start + 24]], axis=0)
            )
    lower_ref[...] = jnp.concatenate(pieces, axis=1).astype(jnp.int32)

    def one_tile(tile):
        lower = lower_ref[pl.ds(tile, 1), :]
        odd = lower % 2
        lanes = pl.ds(pl.multiple_of(tile * 128, 128), 128)
        for parity in range(2):
            order = jnp.where(odd == parity, lower, 4095 - lower)
            factor = jnp.where(order == 0, 1.0, 2.0).astype(F32)
            cosine, sine = cos_sin((order * (512 * row + (255 + shift))) & 16383)
            cos_ref[parity, tile] = cosine * factor
            sin_ref[parity, tile] = -sine * factor
            cos_v, sin_v = cos_sin((order * (2 * row + 1)) & 16383)
            cos_u, sin_u = cos_sin((order * (32 * row[0:8])) & 16383)
            for u in range(8):
                cu = cos_u[u : u + 1, :]
                su = sin_u[u : u + 1, :]
                for part, value in enumerate((cu * cos_v - su * sin_v, su * cos_v + cu * sin_v)):
                    high, low = high_low(value)
                    table_buf[parity, part, 16 * u : 16 * u + 16, lanes] = high
                    table_buf[parity, part, 128 + 16 * u : 144 + 16 * u, lanes] = low

    copies = []
    span = 4
    for block in range(tiles // span):
        pl.loop(block * span, (block + 1) * span)(one_tile)
        for parity in range(2):
            for part in range(2):
                view = (parity, part, slice(None), pl.ds(block * span * 128, span * 128))
                copy = pltpu.make_async_copy(table_buf.at[view], table_ref.at[view], sem.at[len(copies)])
                copy.start()
                copies.append(copy)
    for copy in copies:
        copy.wait()


def tables(cycle_index, slot_orders):
    slots = slot_orders.shape[0]
    vmem = pl.BlockSpec(memory_space=pltpu.VMEM)
    hbm = pl.BlockSpec(memory_space=pltpu.HBM)
    small = jax.ShapeDtypeStruct((2, slots // 128, 16, 128), F32)
    return pl.pallas_call(
        tables_kernel,
        in_specs=[pl.BlockSpec(memory_space=pltpu.SMEM), vmem],
        out_specs=[vmem, vmem, vmem, hbm],
        out_shape=[
            jax.ShapeDtypeStruct((slots // 128, 128), jnp.int32),
            small,
            small,
            jax.ShapeDtypeStruct((2, 2, 256, slots), BF16),
        ],
        scratch_shapes=[
            pltpu.VMEM((2, 2, 256, slots), BF16),
            pltpu.SemaphoreType.DMA((slots // 128,)),
        ],
        compiler_params=pltpu.CompilerParams(vmem_limit_bytes=52 << 20),
        name="tables",
    )(cycle_index, slot_orders.reshape(slots // 128, 128))


def synthesis_kernel(lower_ref, cos_ref, sin_ref, table_ref, sums_ref, out_ref, x_ref, a_ref, table_buf, sem):
    slots = table_ref.shape[3]
    tiles = slots // 128
    copies = [
        pltpu.make_async_copy(
            table_ref.at[parity], table_buf.at[parity, :, :, pl.ds(0, slots)], sem.at[parity]
        )
        for parity in range(2)
    ]
    for copy in copies:
        copy.start()
    for field in range(3):
        for pair in range(2):
            pieces = []
            for middle in range(2):
                for device in range(4):
                    start = device * 12 + field * 4 + pair * 2 + middle
                    pieces.append(sums_ref[pl.ds(start, 16, stride=48), :])
            turned = jnp.concatenate(pieces, axis=0).T
            turned = turned.reshape(8, 16, 128)
            odd = (lower_ref[pair * 8 : pair * 8 + 8, :] % 2 == 1)[:, None, :]
            x_ref[0, field, pair * 8 : pair * 8 + 8] = jnp.where(odd, turned[:, 8:16], turned[:, 0:8])
            x_ref[1, field, pair * 8 : pair * 8 + 8] = jnp.where(odd, turned[:, 0:8], turned[:, 8:16])

    @pl.loop(0, tiles)
    def _(tile):
        lanes = pl.ds(pl.multiple_of(tile * 128, 128), 128)

        @pl.loop(0, 2, unroll=2)
        def _(parity):
            cosine = cos_ref[parity, tile]
            minus = sin_ref[parity, tile]
            for field in range(3):
                x = x_ref[parity, field, tile]
                for comp in range(4):
                    real = x[comp : comp + 1, :]
                    imag = x[4 + comp : 5 + comp, :]
                    rows = (field * 4 + comp) * 16
                    for part, value in enumerate((real * cosine + imag * minus, real * minus - imag * cosine)):
                        high, low = high_low(value)
                        a_ref[parity, part, rows : rows + 16, lanes] = high
                        a_ref[parity, part, 192 + rows : 208 + rows, lanes] = low

    sides = []
    for parity in range(2):
        copies[parity].wait()
        both = []
        for part in range(2):
            wide = lax.dot_general(
                a_ref[parity, part, :, 0:slots], table_buf[parity, part, :, 0:slots], NT, preferred_element_type=F32
            )
            fine = wide[0:192, 128:256] + wide[192:384, 128:256]
            both.append(wide[0:192, 0:128] + (wide[192:384, 0:128] + fine))
        sides.append((both[0] - both[1], both[0] + both[1]))
    for side in range(2):
        lanes = slice(side * 128, side * 128 + 128)
        near = sides[0][side] + sides[1][side]
        far = sides[0][side] - sides[1][side]
        for block in range(4):
            for row in range(12):
                place = slice(row * 4, row * 4 + 4)
                source = slice(row * 16 + block * 4, row * 16 + block * 4 + 4)
                out_ref[block + 4, place, lanes] = near[source, :]
                out_ref[block, place, lanes] = far[source, :]


def synthesis(lower, cosine, sine, table, sums):
    vmem = pl.BlockSpec(memory_space=pltpu.VMEM)
    hbm = pl.BlockSpec(memory_space=pltpu.HBM)
    slots = table.shape[3]
    return pl.pallas_call(
        synthesis_kernel,
        in_specs=[vmem, vmem, vmem, hbm, vmem],
        out_specs=vmem,
        out_shape=jax.ShapeDtypeStruct((8, 48, 256), F32),
        scratch_shapes=[
            pltpu.VMEM((2, 3, slots // 128, 8, 128), F32),
            pltpu.VMEM((2, 2, 384, slots + 128), BF16),
            pltpu.VMEM((2, 2, 256, slots + 128), BF16),
            pltpu.SemaphoreType.DMA((2,)),
        ],
        compiler_params=pltpu.CompilerParams(vmem_limit_bytes=52 << 20),
        name="synthesis",
    )(lower, cosine, sine, table, sums)


def total_kernel(parts_ref, out_ref, sum_ref):
    total = parts_ref[0]
    for source in range(1, 8):
        total = total + parts_ref[source]
    falling = 127 - lax.broadcasted_iota(jnp.int32, (48, 128), 1)
    sum_ref[0] = jnp.take_along_axis(total[:, 0:128], falling, axis=1)
    sum_ref[1] = total[:, 128:256]
    for field in range(3):
        for piece in range(4):
            for side in range(2):
                start = piece * 256 + side * 128
                out_ref[0, field, :, start : start + 128] = sum_ref[side, pl.ds(field * 16 + piece, 4, stride=4), :]


def total(parts):
    vmem = pl.BlockSpec(memory_space=pltpu.VMEM)
    return pl.pallas_call(
        total_kernel,
        in_specs=[vmem],
        out_specs=vmem,
        out_shape=jax.ShapeDtypeStruct((1, 3, 4, 1024), F32),
        scratch_shapes=[pltpu.VMEM((2, 48, 128), F32)],
        compiler_params=pltpu.CompilerParams(vmem_limit_bytes=8 << 20),
        name="total",
    )(parts)


def body(legendre, harmonics, slot_orders, cycle_index):
    sums = legendre_sums(legendre, harmonics, slot_orders)
    swapped = [[device ^ 32 for device in range(64)]]
    moved = lax.all_to_all(
        sums.reshape(64, 3, 4, 128), "ma", split_axis=0, concat_axis=0, axis_index_groups=swapped, tiled=True
    )
    lower, cosine, sine, table = tables(cycle_index, slot_orders)
    blocks = synthesis(lower, cosine, sine, table, moved.reshape(768, 128))
    swapped = [[device ^ 4 for device in range(8)]]
    arrived = lax.all_to_all(
        blocks, "ell", split_axis=0, concat_axis=0, axis_index_groups=swapped, tiled=True
    )
    return total(arrived)


def solution(mesh):
    return jax.shard_map(
        body,
        mesh=mesh,
        in_specs=(P(None, "ma", None, "ell"), P("ma", None, None, None, "ell"), P(), P()),
        out_specs=P("ma", None, None, "ell"),
        check_vma=False,
    )
```

```python
import math

import jax
import jax.numpy as jnp
from jax import lax
from jax.experimental import pallas as pl
from jax.experimental.pallas import tpu as pltpu
from jax.sharding import PartitionSpec as P

F32 = jnp.float32
BF16 = jnp.bfloat16
NT = (((1,), (1,)), ((), ()))


def legendre_kernel(
    orders_hbm, leg_hbm, harm_hbm, out_ref, orders_ref, leg_all, harm_all, pack_ref, acc_ref, sem, orders_sem
):
    groups = leg_hbm.shape[1] // 8
    orders_copy = pltpu.make_async_copy(orders_hbm, orders_ref, orders_sem)
    orders_copy.start()

    def arrivals(group):
        span = pl.ds(group * 8, 8)
        return (
            pltpu.make_async_copy(harm_hbm.at[span], harm_all.at[span], sem.at[0, group]),
            pltpu.make_async_copy(leg_hbm.at[:, span], leg_all.at[:, span], sem.at[1, group]),
        )

    for group in range(groups):
        for copy in arrivals(group):
            copy.start()
    orders_copy.wait()

    @pl.loop(0, groups)
    def _(group):
        for copy in arrivals(group):
            copy.wait()
        span = pl.ds(group * 8, 8)
        legendre_group(
            group, groups, orders_ref, leg_all.at[:, span], harm_all.at[span], out_ref, pack_ref, acc_ref
        )


def legendre_group(group, groups, orders_ref, leg_ref, harm_ref, out_ref, pack_ref, acc_ref):
    pairs = leg_ref.shape[2]
    width = leg_ref.shape[3]
    full = 2 * orders_ref.shape[0]
    first_slot = lax.axis_index("ma") * (8 * groups) + group * 8
    column = lax.axis_index("ell") * width + lax.broadcasted_iota(jnp.int32, (1, width), 1)
    column_sign = (1 - 2 * (column % 2)).astype(F32)
    half = lax.broadcasted_iota(jnp.int32, (8, width), 0) < 4
    upper_rows = lax.broadcasted_iota(jnp.int32, (16, width), 0) >= 8
    for slot in range(8):
        lower = orders_ref[first_slot + slot]
        boundary = full - 1 - lower
        past = column >= boundary
        inside = (column < full - 1) & (past == upper_rows)
        weights = jnp.where(inside, 1.0, 0.0).astype(F32)
        flips = column_sign * jnp.where(upper_rows, (2 * (lower % 2) - 1).astype(F32), 1.0)
        signed = weights * flips
        temp, emode, bmode = (
            jnp.concatenate([harm_ref[slot, kind, part].astype(F32) for part in range(2)], axis=0)
            for kind in range(3)
        )
        eturn = pltpu.roll(emode, 4, 0)
        eturn = jnp.where(half, -eturn, eturn)
        bturn = pltpu.roll(bmode, 4, 0)
        bturn = jnp.where(half, bturn, -bturn)

        def twice(values):
            return jnp.concatenate([values, values], axis=0).astype(BF16)

        temp, emode, bmode = twice(temp), twice(-emode), twice(-bmode)
        eturn, bturn = twice(eturn), twice(bturn)
        for side in range(2):
            straight = (signed if side else weights).astype(BF16)
            turned = (-signed).astype(BF16) if side else straight
            base = side * 32
            pack_ref[slot, base : base + 16, 0:width] = emode * straight
            pack_ref[slot, base : base + 16, width : 2 * width] = bturn * turned
            pack_ref[slot, base + 16 : base + 32, 0:width] = bmode * straight
            pack_ref[slot, base + 16 : base + 32, width : 2 * width] = eturn * turned
            pack_ref[slot, 64 + side * 16 : 80 + side * 16, 0:width] = temp * straight
        both = lax.dot_general(
            jnp.concatenate([leg_ref[1, slot], leg_ref[2, slot]], axis=1),
            pack_ref[slot, 0:64],
            NT,
            preferred_element_type=F32,
        )
        plain = lax.dot_general(
            leg_ref[0, slot], pack_ref[slot, 64:96, 0:width], NT, preferred_element_type=F32
        )
        lanes = slice(16 * slot, 16 * slot + 16)
        for side in range(2):
            acc_ref[side * 3, :, lanes] = plain[:, 16 * side : 16 * side + 16]
            acc_ref[side * 3 + 1, :, lanes] = both[:, 32 * side : 32 * side + 16]
            acc_ref[side * 3 + 2, :, lanes] = both[:, 32 * side + 16 : 32 * side + 32]
    for side in range(2):
        for field in range(3):
            start = (1 - side) * pairs * 12 + field * 4 + group
            out_ref[pl.ds(start, pairs, stride=12), :] = acc_ref[side * 3 + field]


def legendre_sums(legendre, harmonics, orders):
    slots, pairs, width = legendre.shape[1:]
    return pl.pallas_call(
        legendre_kernel,
        in_specs=[pl.BlockSpec(memory_space=pltpu.HBM)] * 3,
        out_specs=pl.BlockSpec(memory_space=pltpu.VMEM),
        scratch_shapes=[
            pltpu.SMEM(orders.shape, jnp.int32),
            pltpu.VMEM((3, slots, pairs, width), BF16),
            pltpu.VMEM(harmonics.shape, BF16),
            pltpu.VMEM((8, 96, 2 * width), BF16),
            pltpu.VMEM((6, pairs, 128), F32),
            pltpu.SemaphoreType.DMA((2, slots // 8)),
            pltpu.SemaphoreType.DMA,
        ],
        out_shape=jax.ShapeDtypeStruct((2 * pairs * 12, 128), F32),
        name="legendre_sums",
    )(orders, legendre, harmonics)


def cos_sin(phase):
    quarter = (phase + 2048) >> 12
    x = (phase - (quarter << 12)).astype(F32) * (math.pi / 8192)
    y = x * x
    sine = x + x * y * (-1.6666667e-1 + y * (8.3333310e-3 + y * (-1.9840874e-4 + y * 2.7525562e-6)))
    cosine = 1.0 + y * (-0.5 + y * (4.16666642e-2 + y * (-1.38887875e-3 + y * 2.4760495e-5)))
    swap = (quarter & 1) == 1
    cos_out = jnp.where(swap, sine, cosine)
    sin_out = jnp.where(swap, cosine, sine)
    cos_flip = ((quarter + 1) & 2) == 2
    sin_flip = (quarter & 2) == 2
    return jnp.where(cos_flip, -cos_out, cos_out), jnp.where(sin_flip, -sin_out, sin_out)


def high_low(value):
    high = value.astype(BF16)
    return high, (value - high.astype(F32)).astype(BF16)


def tables_kernel(cycle_ref, slots_ref, lower_ref, cos_ref, sin_ref, table_ref, table_buf, sem):
    slots = table_ref.shape[3]
    tiles = slots // 128
    shift = cycle_ref[lax.axis_index("ma") % cycle_ref.shape[0]] % 2
    row = lax.broadcasted_iota(jnp.int32, (16, 128), 0)
    turned = jnp.concatenate([slots_ref[8:16, :], slots_ref[0:8, :]], axis=0).astype(F32).T
    pieces = []
    for middle in range(2):
        for device in range(4):
            start = device * 32 + middle * 8
            pieces.append(
                jnp.concatenate([turned[start : start + 8], turned[start + 16 : start + 24]], axis=0)
            )
    lower_ref[...] = jnp.concatenate(pieces, axis=1).astype(jnp.int32)

    def one_tile(tile):
        lower = lower_ref[pl.ds(tile, 1), :]
        odd = lower % 2
        lanes = pl.ds(pl.multiple_of(tile * 128, 128), 128)
        for parity in range(2):
            order = jnp.where(odd == parity, lower, 4095 - lower)
            factor = jnp.where(order == 0, 1.0, 2.0).astype(F32)
            cosine, sine = cos_sin((order * (512 * row + (255 + shift))) & 16383)
            cos_ref[parity, tile] = cosine * factor
            sin_ref[parity, tile] = -sine * factor
            cos_v, sin_v = cos_sin((order * (2 * row + 1)) & 16383)
            cos_u, sin_u = cos_sin((order * (32 * row[0:8])) & 16383)
            for u in range(8):
                cu = cos_u[u : u + 1, :]
                su = sin_u[u : u + 1, :]
                for part, value in enumerate((cu * cos_v - su * sin_v, su * cos_v + cu * sin_v)):
                    high, low = high_low(value)
                    table_buf[parity, part, 16 * u : 16 * u + 16, lanes] = high
                    table_buf[parity, part, 128 + 16 * u : 144 + 16 * u, lanes] = low

    copies = []
    span = 4
    for block in range(tiles // span):
        pl.loop(block * span, (block + 1) * span)(one_tile)
        for parity in range(2):
            for part in range(2):
                view = (parity, part, slice(None), pl.ds(block * span * 128, span * 128))
                copy = pltpu.make_async_copy(table_buf.at[view], table_ref.at[view], sem.at[len(copies)])
                copy.start()
                copies.append(copy)
    for copy in copies:
        copy.wait()


def tables(cycle_index, slot_orders):
    slots = slot_orders.shape[0]
    vmem = pl.BlockSpec(memory_space=pltpu.VMEM)
    hbm = pl.BlockSpec(memory_space=pltpu.HBM)
    small = jax.ShapeDtypeStruct((2, slots // 128, 16, 128), F32)
    return pl.pallas_call(
        tables_kernel,
        in_specs=[pl.BlockSpec(memory_space=pltpu.SMEM), vmem],
        out_specs=[vmem, vmem, vmem, hbm],
        out_shape=[
            jax.ShapeDtypeStruct((slots // 128, 128), jnp.int32),
            small,
            small,
            jax.ShapeDtypeStruct((2, 2, 256, slots), BF16),
        ],
        scratch_shapes=[
            pltpu.VMEM((2, 2, 256, slots), BF16),
            pltpu.SemaphoreType.DMA((slots // 128,)),
        ],
        compiler_params=pltpu.CompilerParams(vmem_limit_bytes=52 << 20),
        name="tables",
    )(cycle_index, slot_orders.reshape(slots // 128, 128))


def synthesis_kernel(lower_ref, cos_ref, sin_ref, table_ref, sums_ref, out_ref, x_ref, a_ref, table_buf, sem):
    slots = table_ref.shape[3]
    tiles = slots // 128
    copies = [
        pltpu.make_async_copy(
            table_ref.at[parity], table_buf.at[parity, :, :, pl.ds(0, slots)], sem.at[parity]
        )
        for parity in range(2)
    ]
    for copy in copies:
        copy.start()
    for field in range(3):
        for pair in range(2):
            pieces = []
            for middle in range(2):
                for device in range(4):
                    start = device * 12 + field * 4 + pair * 2 + middle
                    pieces.append(sums_ref[pl.ds(start, 16, stride=48), :])
            turned = jnp.concatenate(pieces, axis=0).T
            turned = turned.reshape(8, 16, 128)
            odd = (lower_ref[pair * 8 : pair * 8 + 8, :] % 2 == 1)[:, None, :]
            x_ref[0, field, pair * 8 : pair * 8 + 8] = jnp.where(odd, turned[:, 8:16], turned[:, 0:8])
            x_ref[1, field, pair * 8 : pair * 8 + 8] = jnp.where(odd, turned[:, 0:8], turned[:, 8:16])

    @pl.loop(0, tiles)
    def _(tile):
        lanes = pl.ds(pl.multiple_of(tile * 128, 128), 128)

        @pl.loop(0, 2, unroll=2)
        def _(parity):
            cosine = cos_ref[parity, tile]
            minus = sin_ref[parity, tile]
            for field in range(3):
                x = x_ref[parity, field, tile]
                for comp in range(4):
                    real = x[comp : comp + 1, :]
                    imag = x[4 + comp : 5 + comp, :]
                    rows = (field * 4 + comp) * 16
                    for part, value in enumerate((real * cosine + imag * minus, real * minus - imag * cosine)):
                        high, low = high_low(value)
                        a_ref[parity, part, rows : rows + 16, lanes] = high
                        a_ref[parity, part, 192 + rows : 208 + rows, lanes] = low

    sides = []
    for parity in range(2):
        copies[parity].wait()
        both = []
        for part in range(2):
            wide = lax.dot_general(
                a_ref[parity, part, :, 0:slots], table_buf[parity, part, :, 0:slots], NT, preferred_element_type=F32
            )
            fine = wide[0:192, 128:256] + wide[192:384, 128:256]
            both.append(wide[0:192, 0:128] + (wide[192:384, 0:128] + fine))
        sides.append((both[0] - both[1], both[0] + both[1]))
    for side in range(2):
        lanes = slice(side * 128, side * 128 + 128)
        near = sides[0][side] + sides[1][side]
        far = sides[0][side] - sides[1][side]
        for block in range(4):
            for row in range(12):
                place = slice(row * 4, row * 4 + 4)
                source = slice(row * 16 + block * 4, row * 16 + block * 4 + 4)
                out_ref[4 - block, place, lanes] = near[source, :]
                out_ref[-block % 8, place, lanes] = far[source, :]


def synthesis(lower, cosine, sine, table, sums):
    vmem = pl.BlockSpec(memory_space=pltpu.VMEM)
    hbm = pl.BlockSpec(memory_space=pltpu.HBM)
    slots = table.shape[3]
    return pl.pallas_call(
        synthesis_kernel,
        in_specs=[vmem, vmem, vmem, hbm, vmem],
        out_specs=vmem,
        out_shape=jax.ShapeDtypeStruct((8, 48, 256), F32),
        scratch_shapes=[
            pltpu.VMEM((2, 3, slots // 128, 8, 128), F32),
            pltpu.VMEM((2, 2, 384, slots + 128), BF16),
            pltpu.VMEM((2, 2, 256, slots + 128), BF16),
            pltpu.SemaphoreType.DMA((2,)),
        ],
        compiler_params=pltpu.CompilerParams(vmem_limit_bytes=52 << 20),
        name="synthesis",
    )(lower, cosine, sine, table, sums)


def total_kernel(parts_ref, out_ref, sum_ref):
    total = parts_ref[0]
    for source in range(1, 8):
        total = total + parts_ref[source]
    falling = 127 - lax.broadcasted_iota(jnp.int32, (48, 128), 1)
    sum_ref[0] = jnp.take_along_axis(total[:, 0:128], falling, axis=1)
    sum_ref[1] = total[:, 128:256]
    for field in range(3):
        for piece in range(4):
            for side in range(2):
                start = piece * 256 + side * 128
                out_ref[0, field, :, start : start + 128] = sum_ref[side, pl.ds(field * 16 + piece, 4, stride=4), :]


def total(parts):
    vmem = pl.BlockSpec(memory_space=pltpu.VMEM)
    return pl.pallas_call(
        total_kernel,
        in_specs=[vmem],
        out_specs=vmem,
        out_shape=jax.ShapeDtypeStruct((1, 3, 4, 1024), F32),
        scratch_shapes=[pltpu.VMEM((2, 48, 128), F32)],
        compiler_params=pltpu.CompilerParams(vmem_limit_bytes=8 << 20),
        name="total",
    )(parts)


def body(legendre, harmonics, slot_orders, cycle_index):
    sums = legendre_sums(legendre, harmonics, slot_orders)
    swapped = [[device ^ 32 for device in range(64)]]
    moved = lax.all_to_all(
        sums.reshape(64, 3, 4, 128), "ma", split_axis=0, concat_axis=0, axis_index_groups=swapped, tiled=True
    )
    lower, cosine, sine, table = tables(cycle_index, slot_orders)
    blocks = synthesis(lower, cosine, sine, table, moved.reshape(768, 128))
    swapped = [[(4 - rank) % 8 for rank in range(8)]]
    arrived = lax.all_to_all(
        blocks, "ell", split_axis=0, concat_axis=0, axis_index_groups=swapped, tiled=True
    )
    return total(arrived)


def solution(mesh):
    return jax.shard_map(
        body,
        mesh=mesh,
        in_specs=(P(None, "ma", None, "ell"), P("ma", None, None, None, "ell"), P(), P()),
        out_specs=P("ma", None, None, "ell"),
        check_vma=False,
    )
```
